32 devices in a mesh: gx: 2 (over y), gy: 4 (over z), gz: 4 (over x, core).
Axes of the slice: x: 2, y: 2, z: 4, core: 2. Of those that a mesh axis runs over, the one named last changes fastest.
Arguments:
- conserved: float32 [5, 16, 32, 512], P(None, 'gx', 'gy', 'gz'), may hold values from -3 to 4, as said below
- sigma_guess: float32 [16, 32, 512], P('gx', 'gy', 'gz'), may hold values from -30 to 30
Outputs:
- advanced: float32 [5, 16, 32, 512], P(None, 'gx', 'gy', 'gz')
- sigma_field: float32 [16, 32, 512], P('gx', 'gy', 'gz')
The draws below stay inside these ranges and needn't reach their ends.
Inputs may be any that keep to these rules, and one draw needn't show every extreme that they name: `conserved`: component 0 (density) lies between 0.5 and 2, components 1 to 3 (momenta) between -3 and 3, component 4 (energy) between 1 and 4.
All inputs are finite; a program needn't handle non-finite values.
Results may differ from the reference program's by a relative error of at most 0.00002.
Values sent between devices are 32-bit elements; how exact they have to be, the bound alone decides.
A program may use at most 64 MiB of HBM per device.

```python
import jax
import jax.numpy as jnp

SWEEPS = 4
NX = 16
NY = 32
NZ = 512


def draw_conserved(key, part):
    key_rho = jax.random.fold_in(key, 11)
    key_mom = jax.random.fold_in(key, 12)
    key_energy = jax.random.fold_in(key, 13)
    grid_shape = (NX, NY, NZ)
    density = jax.random.uniform(key_rho, grid_shape, jnp.float32, 0.5, 2.0)
    momentum = jnp.clip(0.6 * jax.random.normal(key_mom, (3,) + grid_shape, jnp.float32), -3.0, 3.0)
    energy = jax.random.uniform(key_energy, grid_shape, jnp.float32, 1.0, 2.5)
    return jnp.concatenate([density[None], momentum, energy[None]], axis=0)


def draw_sigma_guess(key, part):
    key_sign = jax.random.fold_in(key, 21)
    key_size = jax.random.fold_in(key, 22)
    grid_shape = (NX, NY, NZ)
    sign_part = (2 * jax.random.randint(key_sign, grid_shape, 0, 2) - 1).astype(jnp.float32)
    magnitude = jax.random.uniform(key_size, grid_shape, jnp.float32, 24.0, 30.0)
    return sign_part * magnitude


def setup_inputs(seed: int = 0) -> dict:
    key_of = jax.random.split(jax.random.key(seed), 3)
    conserved = draw_conserved(jax.random.fold_in(key_of[2], 71), 0)
    sigma_guess = draw_sigma_guess(jax.random.fold_in(key_of[2], 71), 0)
    return dict(conserved=conserved, sigma_guess=sigma_guess)


ALPHA = 10.0
GAMMA = 1.4
LAMBDA = 3.0
STEP_DT = 0.4


def central(field, direction):
    return 0.5 * (jnp.roll(field, -1, direction) - jnp.roll(field, 1, direction))


def source_term(velocity):
    gradient = [[central(velocity[member], across) for across in range(3)] for member in range(3)]
    trace_sq = jnp.zeros_like(velocity[0])
    for member in range(3):
        for across in range(3):
            trace_sq = trace_sq + gradient[member][across] * gradient[across][member]
    divergence = gradient[0][0] + gradient[1][1] + gradient[2][2]
    return trace_sq + divergence * divergence


def jacobi_sweep(sigma_now, inv_density, source):
    acc_num = jnp.zeros_like(sigma_now)
    acc_den = jnp.zeros_like(sigma_now)
    for direction in range(3):
        for offset in (1, -1):
            weight_face = 0.5 * (inv_density + jnp.roll(inv_density, offset, direction))
            acc_num = acc_num + weight_face * jnp.roll(sigma_now, offset, direction)
            acc_den = acc_den + weight_face
    return (ALPHA * source + ALPHA * acc_num) / (inv_density + ALPHA * acc_den)


def physical(states, sigma_face, direction):
    density = states[0]
    normal_speed = states[1 + direction] / density
    kinetic = 0.5 * (states[1] * states[1] + states[2] * states[2] + states[3] * states[3]) / density
    pressure = (GAMMA - 1.0) * (states[4] - kinetic) + sigma_face
    flux_rows = [states[1 + direction]]
    for member in range(3):
        flux_term = states[1 + member] * normal_speed
        if member == direction:
            flux_term = flux_term + pressure
        flux_rows.append(flux_term)
    flux_rows.append((states[4] + pressure) * normal_speed)
    return jnp.stack(flux_rows)


def flux_change(conserved, sigma_field, direction):
    axis_q = direction + 1
    left_state = (5.0 * conserved + 2.0 * jnp.roll(conserved, -1, axis_q) - jnp.roll(conserved, 1, axis_q)) / 6.0
    right_state = (2.0 * conserved + 5.0 * jnp.roll(conserved, -1, axis_q) - jnp.roll(conserved, -2, axis_q)) / 6.0
    left_sigma = (5.0 * sigma_field + 2.0 * jnp.roll(sigma_field, -1, direction) - jnp.roll(sigma_field, 1, direction)) / 6.0
    right_sigma = (2.0 * sigma_field + 5.0 * jnp.roll(sigma_field, -1, direction) - jnp.roll(sigma_field, -2, direction)) / 6.0
    face_flux = 0.5 * (physical(left_state, left_sigma, direction) + physical(right_state, right_sigma, direction)) - 0.5 * LAMBDA * (right_state - left_state)
    return face_flux - jnp.roll(face_flux, 1, axis_q)


def reference(conserved, sigma_guess):
    inv_density = 1.0 / conserved[0]
    velocity = conserved[1:4] / conserved[0]
    source = source_term(velocity)
    sigma_now = sigma_guess
    for sweep_no in range(SWEEPS):
        sigma_now = jacobi_sweep(sigma_now, inv_density, source)
    tendency = jnp.zeros_like(conserved)
    for direction in range(3):
        tendency = tendency - flux_change(conserved, sigma_now, direction)
    advanced = conserved + STEP_DT * tendency
    return advanced, sigma_now
```

```python
import functools
import itertools

import jax
import jax.numpy as jnp
from jax import lax
from jax.experimental import pallas as pl
from jax.experimental.pallas import tpu as pltpu
from jax.sharding import PartitionSpec as P

SWEEPS = 4
ALPHA = 10.0
GAMMA = 1.4
LAMBDA = 3.0
STEP_DT = 0.4
MESH = pl.DeviceIdType.MESH
AXES = ("gx", "gy", "gz")

OFFSETS = [o for o in itertools.product((-1, 0, 1), repeat=3) if 1 <= sum(abs(v) for v in o) <= 2]
NEAR = [o for o in OFFSETS if sum(abs(v) for v in o) == 1]
Z_MOVES = [o for o in OFFSETS if o[2] != 0]
XY_MOVES = [o for o in OFFSETS if o[0] != 0 and o[1] != 0]


def neg(offset):
    return tuple(-v for v in offset)


def iota(shape, dim):
    return lax.broadcasted_iota(jnp.int32, shape, dim)


def roll(value, shift, axis):
    size = value.shape[axis]
    shift = shift % size
    return value if shift == 0 else pltpu.roll(value, shift, axis)


def ring(core, ghost, step, axis):
    size = core.shape[axis]
    a, b = roll(core, -step, axis), roll(ghost, -step, axis)
    edge = iota(core.shape, axis) == (size - 1 if step == 1 else 0)
    return jnp.where(edge, b, a), jnp.where(edge, a, b)


def kernel(sizes, cons_hbm, sig_hbm, adv_ref, out_sig_ref, cons, sig,
           y1s, z1s, d1s, xm1r, xs1r, y1r, z1r, d1r,
           s2, y2s, z2s, x2r, y2r, z2r, d2r,
           y3s, z3s, x3r, y3r, z3r,
           in_sem, send_sem, recv_sem):
    X, R, L = sig.shape
    me = [lax.axis_index(a) for a in AXES]
    G = X // 4

    def device(offset):
        return {a: lax.rem(me[i] + offset[i] + sizes[i], sizes[i]) for i, a in enumerate(AXES)}

    load_c = pltpu.make_async_copy(cons_hbm, cons, in_sem.at[0])
    load_s = pltpu.make_async_copy(sig_hbm, sig, in_sem.at[1])
    load_c.start()
    load_s.start()
    barrier = pltpu.get_barrier_semaphore()
    for o in OFFSETS:
        pl.semaphore_signal(barrier, inc=1, device_id=device(o), device_id_type=MESH)

    sent = []
    count = [0]

    def send(src, dst, offset):
        n = count[0]
        count[0] += 1
        copy = pltpu.make_async_remote_copy(
            src_ref=src, dst_ref=dst, send_sem=send_sem.at[n], recv_sem=recv_sem.at[n],
            device_id=device(offset), device_id_type=MESH)
        copy.start()
        sent.append(copy)
        return copy

    rows = lambda shape: iota(shape, len(shape) - 2)
    lanes = lambda shape: iota(shape, len(shape) - 1)

    def pack_rows(field, first):
        out = field[0:G]
        r = rows(out.shape)
        for g in range(1, 4):
            part = roll(field[g * G:(g + 1) * G], 2 * g, 1)
            at = (first + 2 * g) % R
            out = jnp.where((r == at) | (r == at + 1), part, out)
        return out

    def unpack_rows(after, before):
        parts = []
        low = rows(after.shape) < R // 2
        for g in range(4):
            parts.append(jnp.where(low, roll(after, -2 * g, 1), roll(before, -2 * g, 1)))
        return jnp.concatenate(parts, axis=0)

    def pack_lanes(fields):
        tiles = [f[p] for f in fields for p in range(X)]
        out = jnp.zeros((R, L), jnp.float32)
        lane = lanes((R, L))
        for k, tile in enumerate(tiles):
            out = jnp.where(((lane + 2) % L) // 4 == k, roll(tile, 4 * k, 1), out)
        return out

    def merge_lanes(after, before):
        return jnp.where(lanes(after.shape) % 4 < 2, after, before)

    def unpack_lanes(packed, k):
        return roll(packed, -4 * k, 1)

    load_c.wait()
    load_s.wait()
    pl.semaphore_wait(barrier, len(OFFSETS))
    x1 = []
    for j, (dx, lo) in enumerate(((1, X - 2), (-1, 0))):
        x1.append(send(cons.at[0:4, lo:lo + 2], xm1r.at[j, 0:4], (dx, 0, 0)))
        x1.append(send(sig.at[lo:lo + 2], xs1r.at[j], (dx, 0, 0)))
    C0 = [cons[f] for f in range(4)] + [sig[...], cons[4]]
    for f in range(5):
        y1s[0, f] = pack_rows(C0[f], R - 2)
        y1s[1, f] = pack_rows(C0[f], 0)
    y1 = []
    for j, dy in enumerate((1, -1)):
        y1.append(send(y1s.at[j, 0:5], y1r.at[j, 0:5], (0, dy, 0)))
    z1s[0] = pack_lanes(C0[0:4])
    z1s[1] = pack_lanes(C0[4:6])
    row2 = rows((R, L))
    for n, (dx, dy, _) in enumerate(XY_MOVES):
        p = X - 1 if dx == 1 else 0
        src = R - 1 if dy == 1 else 0
        out = C0[0][p]
        for f in range(1, 5):
            out = jnp.where(row2 == (src + f) % R, roll(C0[f][p], f, 0), out)
        d1s[n] = out
    d1 = [send(d1s.at[n], d1r.at[n], o) for n, o in enumerate(XY_MOVES)]
    z1 = [send(z1s, z1r.at[n], o) for n, o in enumerate(Z_MOVES)]
    late = []
    for j, (dx, lo) in enumerate(((1, X - 2), (-1, 0))):
        late.append(send(cons.at[4, lo:lo + 2], xm1r.at[j, 4], (dx, 0, 0)))
    y1s[0, 5] = pack_rows(C0[5], R - 2)
    y1s[1, 5] = pack_rows(C0[5], 0)
    for j, dy in enumerate((1, -1)):
        late.append(send(y1s.at[j, 5], y1r.at[j, 5], (0, dy, 0)))
    for copy in x1 + y1 + d1 + z1:
        copy.wait_recv()

    def z_from(buf, dx, dy):
        return merge_lanes(buf[Z_MOVES.index((-dx, -dy, -1))], buf[Z_MOVES.index((-dx, -dy, 1))])

    def grown(core, xlo, xhi, y, zpack, f, dlo, dhi):
        c = jnp.concatenate([xlo, core, xhi], axis=0)
        y = jnp.concatenate([dlo[None], y, dhi[None]], axis=0)
        here, below, above, diag = zpack
        z = [unpack_lanes(below, f * X + X - 1)]
        z += [unpack_lanes(here, f * X + p) for p in range(X)]
        z += [unpack_lanes(above, f * X)]
        w = [unpack_lanes(diag, f * X + p) for p in range(X)]
        stack = lambda t: jnp.concatenate([v[None] for v in t], axis=0)
        return c, y, stack(z), stack(w)

    def z_packs(buf):
        low = rows(buf.shape[1:]) < R // 2
        return (z_from(buf, 0, 0), z_from(buf, -1, 0), z_from(buf, 1, 0),
                jnp.where(low, z_from(buf, 0, 1), z_from(buf, 0, -1)))

    packs = z_packs(z1r)
    low2 = row2 < R // 2

    def corner(buf, dx, f):
        after = buf[XY_MOVES.index((-dx, -1, 0))]
        before = buf[XY_MOVES.index((-dx, 1, 0))]
        return jnp.where(low2, roll(after, -f, 0), roll(before, -f, 0))

    ext = []
    for f in range(5):
        zp = tuple(v[0 if f < 4 else 1] for v in packs)
        xlo, xhi = (xm1r[0, f], xm1r[1, f]) if f < 4 else (xs1r[0], xs1r[1])
        yy = unpack_rows(y1r[1, f], y1r[0, f])
        ext.append(grown(C0[f], xlo, xhi, yy, zp, f % 4, corner(d1r, -1, f), corner(d1r, 1, f)))

    def around(field):
        c, y, z, w = field
        cm = c[1:X + 3]
        yp, ym = ring(cm, y, 1, 1), ring(cm, y, -1, 1)
        zp, zm = ring(cm, z, 1, 2), ring(cm, z, -1, 2)
        zy_p, zy_m = ring(z[1:X + 1], w, 1, 1)[0], ring(z[1:X + 1], w, -1, 1)[0]
        yz_p, yz_m = ring(y[1:X + 1], w, 1, 2)[0], ring(y[1:X + 1], w, -1, 2)[0]
        core = [(c[2:X + 4], c[0:X + 2]), (yp[0], ym[0]), (zp[0], zm[0])]
        yt = [(y[2:X + 2], y[0:X]), (yp[1][1:X + 1], ym[1][1:X + 1]), (yz_p, yz_m)]
        zt = [(z[2:X + 2], z[0:X]), (zy_p, zy_m), (zp[1][1:X + 1], zm[1][1:X + 1])]
        return core, yt, zt

    def middle(field):
        c, y, z, _ = field
        return c[1:X + 3], y[1:X + 1], z[1:X + 1]

    inv = tuple(1.0 / v for v in ext[0])
    vel = [tuple(m * r for m, r in zip(ext[k], inv)) for k in (1, 2, 3)]
    vel_n = [around(v) for v in vel]
    inv_n = around(inv)
    inv_m = middle(inv)
    source, weight, scale = [], [], []
    for t in range(3):
        g = [[0.5 * (vel_n[k][t][d][0] - vel_n[k][t][d][1]) for d in range(3)] for k in range(3)]
        div = g[0][0] + g[1][1] + g[2][2]
        source.append(g[0][0] * g[0][0] + g[1][1] * g[1][1] + g[2][2] * g[2][2]
                      + 2.0 * (g[0][1] * g[1][0] + g[0][2] * g[2][0] + g[1][2] * g[2][1]) + div * div)
        ws = [[0.5 * (inv_m[t] + inv_n[t][d][s]) for s in range(2)] for d in range(3)]
        total = sum(w for pair in ws for w in pair)
        weight.append(ws)
        scale.append(ALPHA / (inv_m[t] + ALPHA * total))

    def update(nbr, t, cut=None):
        take = (lambda v: v) if cut is None else (lambda v: v[cut])
        acc = take(source[t])
        for d in range(3):
            for s in range(2):
                acc = acc + take(weight[t][d][s]) * nbr[d][s]
        return acc * take(scale[t])

    def core_sweep(c, y, z):
        m = c[1:X + 1]
        nbr = [(c[2:X + 2], c[0:X]),
               (ring(m, y, 1, 1)[0], ring(m, y, -1, 1)[0]),
               (ring(m, z, 1, 2)[0], ring(m, z, -1, 2)[0])]
        return update(nbr, 0, slice(1, X + 1))

    def two_sweeps(field):
        n = around(field)
        c, y, z = (update(n[t], t) for t in range(3))
        return core_sweep(c, y, z)

    sigma2 = two_sweeps(ext[4])
    s2[...] = sigma2
    y2s[0] = pack_rows(sigma2, R - 2)
    y2s[1] = pack_rows(sigma2, 0)
    z2s[...] = pack_lanes([sigma2])
    got2 = []
    for j, dy in enumerate((1, -1)):
        got2.append(send(y2s.at[j], y2r.at[j], (0, dy, 0)))
    for n, o in enumerate(XY_MOVES):
        got2.append(send(s2.at[X - 1 if o[0] == 1 else 0], d2r.at[n], o))
    for n, o in enumerate(Z_MOVES):
        got2.append(send(z2s, z2r.at[n], o))
    for j, (dx, lo) in enumerate(((1, X - 2), (-1, 0))):
        got2.append(send(s2.at[lo:lo + 2], x2r.at[j], (dx, 0, 0)))

    for copy in late:
        copy.wait_recv()
    order = (0, 1, 2, 3)
    xc = [ext[f][0] for f in order] + [jnp.concatenate([xm1r[0, 4], C0[5], xm1r[1, 4]], axis=0)]
    yc = [ext[f][1][1:X + 1] for f in order] + [unpack_rows(y1r[1, 5], y1r[0, 5])]
    zc = [ext[f][2][1:X + 1] for f in order] + [
        jnp.concatenate([unpack_lanes(packs[0][1], X + p)[None] for p in range(X)], axis=0)]
    core = C0[0:4] + [C0[5]]

    def x_stencil(c):
        return c[0:X + 1], c[1:X + 2], c[2:X + 3], c[3:X + 4]

    def ring_stencil(c, g, axis):
        m, p = ring(c, g, -1, axis), ring(c, g, 1, axis)
        pp = ring(p[0], p[1], 1, axis)
        cat = lambda a, b: jnp.concatenate([a, b], axis=0)
        return cat(*m), cat(c, g), cat(*p), cat(*pp)

    def faces(st):
        m, q, p, pp = st
        sixth = 1.0 / 6.0
        return (5.0 * q + 2.0 * p - m) * sixth, (2.0 * q + 5.0 * p - pp) * sixth

    def plain_flux(s, d):
        r = 1.0 / s[0]
        v = s[1 + d] * r
        pressure = (GAMMA - 1.0) * (s[4] - 0.5 * (s[1] * s[1] + s[2] * s[2] + s[3] * s[3]) * r)
        out = [s[1 + d]]
        for k in range(3):
            out.append(s[1 + k] * v + pressure if k == d else s[1 + k] * v)
        out.append((s[4] + pressure) * v)
        return out, v

    def difference(flux, d):
        if d == 0:
            return flux[1:X + 1] - flux[0:X]
        return flux[0:X] - ring(flux[0:X], flux[X:2 * X], -1, d)[0]

    base = [None] * 5
    speed = []
    for d in range(3):
        if d == 0:
            lr = [faces(x_stencil(c)) for c in xc]
        else:
            lr = [faces(ring_stencil(c, g, d)) for c, g in zip(core, (None, yc, zc)[d])]
        lf, lv = plain_flux([v[0] for v in lr], d)
        rf, rv = plain_flux([v[1] for v in lr], d)
        speed.append((lv, rv))
        for k in range(5):
            flux = 0.5 * (lf[k] + rf[k]) - (0.5 * LAMBDA) * (lr[k][1] - lr[k][0])
            change = difference(flux, d)
            base[k] = change if base[k] is None else base[k] + change
    base = [core[k] - STEP_DT * base[k] for k in range(5)]
    adv_ref[0] = base[0]

    for copy in got2:
        copy.wait_recv()
    zp2 = z_packs(z2r)
    c2 = jnp.concatenate([x2r[0], sigma2, x2r[1]], axis=0)
    sigma4 = two_sweeps(grown(sigma2, x2r[0], x2r[1], unpack_rows(y2r[1], y2r[0]), zp2, 0,
                              corner(d2r, -1, 0), corner(d2r, 1, 0)))

    out_sig_ref[...] = sigma4
    y3s[0] = pack_rows(sigma4, R - 2)
    y3s[1] = pack_rows(sigma4, 0)
    z3s[...] = pack_lanes([sigma4])
    got3 = []
    for j, dy in enumerate((1, -1)):
        got3.append(send(y3s.at[j], y3r.at[j], (0, dy, 0)))
    for j, dz in enumerate((1, -1)):
        got3.append(send(z3s, z3r.at[j], (0, 0, dz)))
    for j, (dx, lo) in enumerate(((1, X - 2), (-1, 0))):
        got3.append(send(out_sig_ref.at[lo:lo + 2], x3r.at[j], (dx, 0, 0)))
    for copy in got3:
        copy.wait_recv()
    y3 = unpack_rows(y3r[1], y3r[0])
    zpk = merge_lanes(z3r[1], z3r[0])
    z3 = jnp.concatenate([unpack_lanes(zpk, p)[None] for p in range(X)], axis=0)
    x3 = jnp.concatenate([x3r[0], sigma4, x3r[1]], axis=0)
    energy = base[4]
    for d in range(3):
        st = x_stencil(x3) if d == 0 else ring_stencil(sigma4, y3 if d == 1 else z3, d)
        ls, rs = faces(st)
        lv, rv = speed[d]
        adv_ref[1 + d] = base[1 + d] - (0.5 * STEP_DT) * difference(ls + rs, d)
        energy = energy - (0.5 * STEP_DT) * difference(ls * lv + rs * rv, d)
    adv_ref[4] = energy
    for copy in sent:
        copy.wait_send()


def solution(mesh):
    sizes = tuple(mesh.shape[a] for a in AXES)

    def on_device(conserved, sigma_guess):
        X, R, L = sigma_guess.shape
        G = X // 4
        f32 = jnp.float32
        vm = lambda *shape: pltpu.VMEM(shape, f32)
        nz, nd = len(Z_MOVES), len(XY_MOVES)
        messages = 48
        return pl.pallas_call(
            functools.partial(kernel, sizes),
            out_shape=(jax.ShapeDtypeStruct(conserved.shape, f32), jax.ShapeDtypeStruct(sigma_guess.shape, f32)),
            in_specs=[pl.BlockSpec(memory_space=pl.ANY)] * 2,
            out_specs=(pl.BlockSpec(memory_space=pltpu.VMEM),) * 2,
            scratch_shapes=[
                vm(*conserved.shape), vm(X, R, L),
                vm(2, 6, G, R, L), vm(2, R, L), vm(nd, R, L),
                vm(2, 5, 2, R, L), vm(2, 2, R, L), vm(2, 6, G, R, L), vm(nz, 2, R, L), vm(nd, R, L),
                vm(X, R, L), vm(2, G, R, L), vm(R, L),
                vm(2, 2, R, L), vm(2, G, R, L), vm(nz, R, L), vm(nd, R, L),
                vm(2, G, R, L), vm(R, L),
                vm(2, 2, R, L), vm(2, G, R, L), vm(2, R, L),
                pltpu.SemaphoreType.DMA((2,)),
                pltpu.SemaphoreType.DMA((messages,)),
                pltpu.SemaphoreType.DMA((messages,)),
            ],
            compiler_params=pltpu.CompilerParams(collective_id=0, has_side_effects=True),
        )(conserved, sigma_guess)

    specs = (P(None, "gx", "gy", "gz"), P("gx", "gy", "gz"))
    return jax.shard_map(on_device, mesh=mesh, in_specs=specs, out_specs=specs, check_vma=False)
```

```python
import functools
import itertools

import jax
import jax.numpy as jnp
from jax import lax
from jax.experimental import pallas as pl
from jax.experimental.pallas import tpu as pltpu
from jax.sharding import PartitionSpec as P

SWEEPS = 4
ALPHA = 10.0
GAMMA = 1.4
LAMBDA = 3.0
STEP_DT = 0.4
MESH = pl.DeviceIdType.MESH
AXES = ("gx", "gy", "gz")

OFFSETS = [o for o in itertools.product((-1, 0, 1), repeat=3) if 1 <= sum(abs(v) for v in o) <= 2]
NEAR = [o for o in OFFSETS if sum(abs(v) for v in o) == 1]
Z_MOVES = [o for o in OFFSETS if o[2] != 0]
XY_MOVES = [o for o in OFFSETS if o[0] != 0 and o[1] != 0]


def neg(offset):
    return tuple(-v for v in offset)


def iota(shape, dim):
    return lax.broadcasted_iota(jnp.int32, shape, dim)


def roll(value, shift, axis):
    size = value.shape[axis]
    shift = shift % size
    return value if shift == 0 else pltpu.roll(value, shift, axis)


def ring(core, ghost, step, axis):
    size = core.shape[axis]
    a, b = roll(core, -step, axis), roll(ghost, -step, axis)
    edge = iota(core.shape, axis) == (size - 1 if step == 1 else 0)
    return jnp.where(edge, b, a), jnp.where(edge, a, b)


def kernel(sizes, cons_hbm, sig_hbm, adv_ref, out_sig_ref, cons, sig,
           y1s, z1s, d1s, xm1r, xs1r, y1r, z1r, d1r,
           s2, y2s, z2s, x2r, y2r, z2r, d2r,
           y3s, z3s, x3r, y3r, z3r,
           in_sem, send_sem, recv_sem):
    X, R, L = sig.shape
    me = [lax.axis_index(a) for a in AXES]
    G = X // 4

    def device(offset):
        return {a: lax.rem(me[i] + offset[i] + sizes[i], sizes[i]) for i, a in enumerate(AXES)}

    load_c = pltpu.make_async_copy(cons_hbm, cons, in_sem.at[0])
    load_s = pltpu.make_async_copy(sig_hbm, sig, in_sem.at[1])
    load_c.start()
    load_s.start()
    barrier = pltpu.get_barrier_semaphore()
    for o in OFFSETS:
        pl.semaphore_signal(barrier, inc=1, device_id=device(o), device_id_type=MESH)

    sent = []
    count = [0]

    def send(src, dst, offset):
        n = count[0]
        count[0] += 1
        copy = pltpu.make_async_remote_copy(
            src_ref=src, dst_ref=dst, send_sem=send_sem.at[n], recv_sem=recv_sem.at[n],
            device_id=device(offset), device_id_type=MESH)
        copy.start()
        sent.append(copy)
        return copy

    rows = lambda shape: iota(shape, len(shape) - 2)
    lanes = lambda shape: iota(shape, len(shape) - 1)

    def pack_rows(field, first):
        out = field[0:G]
        r = rows(out.shape)
        for g in range(1, 4):
            part = roll(field[g * G:(g + 1) * G], 2 * g, 1)
            at = (first + 2 * g) % R
            out = jnp.where((r == at) | (r == at + 1), part, out)
        return out

    def unpack_rows(after, before):
        parts = []
        low = rows(after.shape) < R // 2
        for g in range(4):
            parts.append(jnp.where(low, roll(after, -2 * g, 1), roll(before, -2 * g, 1)))
        return jnp.concatenate(parts, axis=0)

    def pack_lanes(fields):
        tiles = [f[p] for f in fields for p in range(X)]
        out = jnp.zeros((R, L), jnp.float32)
        lane = lanes((R, L))
        for k, tile in enumerate(tiles):
            out = jnp.where(((lane + 2) % L) // 4 == k, roll(tile, 4 * k, 1), out)
        return out

    def merge_lanes(after, before):
        return jnp.where(lanes(after.shape) % 4 < 2, after, before)

    def unpack_lanes(packed, k):
        return roll(packed, -4 * k, 1)

    load_c.wait()
    load_s.wait()
    pl.semaphore_wait(barrier, len(OFFSETS))
    x1 = []
    for j, (dx, lo) in enumerate(((1, X - 2), (-1, 0))):
        x1.append(send(cons.at[0:4, lo:lo + 2], xm1r.at[j, 0:4], (dx, 0, 0)))
        x1.append(send(sig.at[lo:lo + 2], xs1r.at[j], (dx, 0, 0)))
    C0 = [cons[f] for f in range(4)] + [sig[...], cons[4]]
    for f in range(5):
        y1s[0, f] = pack_rows(C0[f], R - 2)
        y1s[1, f] = pack_rows(C0[f], 0)
    y1 = []
    for j, dy in enumerate((1, -1)):
        y1.append(send(y1s.at[j, 0:5], y1r.at[j, 0:5], (0, dy, 0)))
    z1s[0] = pack_lanes(C0[0:4])
    z1s[1] = pack_lanes(C0[4:6])
    row2 = rows((R, L))
    for n, (dx, dy, _) in enumerate(XY_MOVES):
        p = X - 1 if dx == 1 else 0
        src = R - 1 if dy == 1 else 0
        out = C0[0][p]
        for f in range(1, 5):
            out = jnp.where(row2 == (src + f) % R, roll(C0[f][p], f, 0), out)
        d1s[n] = out
    d1 = [send(d1s.at[n], d1r.at[n], o) for n, o in enumerate(XY_MOVES)]
    z1 = [send(z1s, z1r.at[n], o) for n, o in enumerate(Z_MOVES)]
    late = []
    for j, (dx, lo) in enumerate(((1, X - 2), (-1, 0))):
        late.append(send(cons.at[4, lo:lo + 2], xm1r.at[j, 4], (dx, 0, 0)))
    y1s[0, 5] = pack_rows(C0[5], R - 2)
    y1s[1, 5] = pack_rows(C0[5], 0)
    for j, dy in enumerate((1, -1)):
        late.append(send(y1s.at[j, 5], y1r.at[j, 5], (0, dy, 0)))
    for copy in x1 + y1 + d1 + z1:
        copy.wait_recv()

    def z_from(buf, dx, dy):
        return merge_lanes(buf[Z_MOVES.index((-dx, -dy, -1))], buf[Z_MOVES.index((-dx, -dy, 1))])

    def grown(core, xlo, xhi, y, zpack, f, dlo, dhi):
        c = jnp.concatenate([xlo, core, xhi], axis=0)
        y = jnp.concatenate([dlo[None], y, dhi[None]], axis=0)
        here, below, above, diag = zpack
        z = [unpack_lanes(below, f * X + X - 1)]
        z += [unpack_lanes(here, f * X + p) for p in range(X)]
        z += [unpack_lanes(above, f * X)]
        w = [unpack_lanes(diag, f * X + p) for p in range(X)]
        stack = lambda t: jnp.concatenate([v[None] for v in t], axis=0)
        return c, y, stack(z), stack(w)

    def z_packs(buf):
        low = rows(buf.shape[1:]) < R // 2
        return (z_from(buf, 0, 0), z_from(buf, -1, 0), z_from(buf, 1, 0),
                jnp.where(low, z_from(buf, 0, 1), z_from(buf, 0, -1)))

    packs = z_packs(z1r)
    low2 = row2 < R // 2

    def corner(buf, dx, f):
        after = buf[XY_MOVES.index((-dx, -1, 0))]
        before = buf[XY_MOVES.index((-dx, 1, 0))]
        return jnp.where(low2, roll(after, -f, 0), roll(before, -f, 0))

    ext = []
    for f in range(5):
        zp = tuple(v[0 if f < 4 else 1] for v in packs)
        xlo, xhi = (xm1r[0, f], xm1r[1, f]) if f < 4 else (xs1r[0], xs1r[1])
        yy = unpack_rows(y1r[1, f], y1r[0, f])
        ext.append(grown(C0[f], xlo, xhi, yy, zp, f % 4, corner(d1r, -1, f), corner(d1r, 1, f)))

    def around(field):
        c, y, z, w = field
        cm = c[1:X + 3]
        yp, ym = ring(cm, y, 1, 1), ring(cm, y, -1, 1)
        zp, zm = ring(cm, z, 1, 2), ring(cm, z, -1, 2)
        zy_p, zy_m = ring(z[1:X + 1], w, 1, 1)[0], ring(z[1:X + 1], w, -1, 1)[0]
        yz_p, yz_m = ring(y[1:X + 1], w, 1, 2)[0], ring(y[1:X + 1], w, -1, 2)[0]
        core = [(c[2:X + 4], c[0:X + 2]), (yp[0], ym[0]), (zp[0], zm[0])]
        yt = [(y[2:X + 2], y[0:X]), (yp[1][1:X + 1], ym[1][1:X + 1]), (yz_p, yz_m)]
        zt = [(z[2:X + 2], z[0:X]), (zy_p, zy_m), (zp[1][1:X + 1], zm[1][1:X + 1])]
        return core, yt, zt

    def middle(field):
        c, y, z, _ = field
        return c[1:X + 3], y[1:X + 1], z[1:X + 1]

    inv = tuple(1.0 / v for v in ext[0])
    vel = [tuple(m * r for m, r in zip(ext[k], inv)) for k in (1, 2, 3)]
    vel_n = [around(v) for v in vel]
    inv_n = around(inv)
    inv_m = middle(inv)
    source, weight, scale = [], [], []
    for t in range(3):
        g = [[0.5 * (vel_n[k][t][d][0] - vel_n[k][t][d][1]) for d in range(3)] for k in range(3)]
        div = g[0][0] + g[1][1] + g[2][2]
        source.append(g[0][0] * g[0][0] + g[1][1] * g[1][1] + g[2][2] * g[2][2]
                      + 2.0 * (g[0][1] * g[1][0] + g[0][2] * g[2][0] + g[1][2] * g[2][1]) + div * div)
        ws = [[0.5 * (inv_m[t] + inv_n[t][d][s]) for s in range(2)] for d in range(3)]
        total = sum(w for pair in ws for w in pair)
        weight.append(ws)
        scale.append(ALPHA / (inv_m[t] + ALPHA * total))

    def update(nbr, t, cut=None):
        take = (lambda v: v) if cut is None else (lambda v: v[cut])
        acc = take(source[t])
        for d in range(3):
            for s in range(2):
                acc = acc + take(weight[t][d][s]) * nbr[d][s]
        return acc * take(scale[t])

    def core_sweep(c, y, z):
        m = c[1:X + 1]
        nbr = [(c[2:X + 2], c[0:X]),
               (ring(m, y, 1, 1)[0], ring(m, y, -1, 1)[0]),
               (ring(m, z, 1, 2)[0], ring(m, z, -1, 2)[0])]
        return update(nbr, 0, slice(1, X + 1))

    def two_sweeps(field):
        n = around(field)
        c, y, z = (update(n[t], t) for t in range(3))
        return core_sweep(c, y, z)

    sigma2 = two_sweeps(ext[4])
    s2[...] = sigma2
    y2s[0] = pack_rows(sigma2, R - 2)
    y2s[1] = pack_rows(sigma2, 0)
    z2s[...] = pack_lanes([sigma2])
    got2 = []
    for j, dy in enumerate((1, -1)):
        got2.append(send(y2s.at[j], y2r.at[j], (0, dy, 0)))
    for n, o in enumerate(XY_MOVES):
        got2.append(send(s2.at[X - 1 if o[0] == 1 else 0], d2r.at[n], o))
    for n, o in enumerate(Z_MOVES):
        got2.append(send(z2s, z2r.at[n], o))
    for j, (dx, lo) in enumerate(((1, X - 2), (-1, 0))):
        got2.append(send(s2.at[lo:lo + 2], x2r.at[j], (dx, 0, 0)))

    for copy in late:
        copy.wait_recv()
    order = (0, 1, 2, 3)
    xc = [ext[f][0] for f in order] + [jnp.concatenate([xm1r[0, 4], C0[5], xm1r[1, 4]], axis=0)]
    yc = [ext[f][1][1:X + 1] for f in order] + [unpack_rows(y1r[1, 5], y1r[0, 5])]
    zc = [ext[f][2][1:X + 1] for f in order] + [
        jnp.concatenate([unpack_lanes(packs[0][1], X + p)[None] for p in range(X)], axis=0)]
    core = C0[0:4] + [C0[5]]

    def x_stencil(c):
        return c[0:X + 1], c[1:X + 2], c[2:X + 3], c[3:X + 4]

    def ring_stencil(c, g, axis):
        m, p = ring(c, g, -1, axis), ring(c, g, 1, axis)
        pp = ring(p[0], p[1], 1, axis)
        cat = lambda a, b: jnp.concatenate([a, b], axis=0)
        return cat(*m), cat(c, g), cat(*p), cat(*pp)

    def faces(st):
        m, q, p, pp = st
        sixth = 1.0 / 6.0
        return (5.0 * q + 2.0 * p - m) * sixth, (2.0 * q + 5.0 * p - pp) * sixth

    def plain_flux(s, d):
        r = 1.0 / s[0]
        v = s[1 + d] * r
        pressure = (GAMMA - 1.0) * (s[4] - 0.5 * (s[1] * s[1] + s[2] * s[2] + s[3] * s[3]) * r)
        out = [s[1 + d]]
        for k in range(3):
            out.append(s[1 + k] * v + pressure if k == d else s[1 + k] * v)
        out.append((s[4] + pressure) * v)
        return out, v

    def difference(flux, d):
        if d == 0:
            return flux[1:X + 1] - flux[0:X]
        return flux[0:X] - ring(flux[0:X], flux[X:2 * X], -1, d)[0]

    base = [None] * 5
    speed = []
    for d in range(3):
        if d == 0:
            lr = [faces(x_stencil(c)) for c in xc]
        else:
            lr = [faces(ring_stencil(c, g, d)) for c, g in zip(core, (None, yc, zc)[d])]
        lf, lv = plain_flux([v[0] for v in lr], d)
        rf, rv = plain_flux([v[1] for v in lr], d)
        speed.append((lv, rv))
        for k in range(5):
            flux = 0.5 * (lf[k] + rf[k]) - (0.5 * LAMBDA) * (lr[k][1] - lr[k][0])
            change = difference(flux, d)
            base[k] = change if base[k] is None else base[k] + change
    base = [core[k] - STEP_DT * base[k] for k in range(5)]
    adv_ref[0] = base[0]

    for copy in got2:
        copy.wait_recv()
    zp2 = z_packs(z2r)
    c2 = jnp.concatenate([x2r[0], sigma2, x2r[1]], axis=0)
    sigma4 = two_sweeps(grown(sigma2, x2r[0], x2r[1], unpack_rows(y2r[1], y2r[0]), zp2, 0,
                              corner(d2r, -1, 0), corner(d2r, 1, 0)))

    out_sig_ref[...] = sigma4
    y3s[0] = pack_rows(sigma4, R - 2)
    y3s[1] = pack_rows(sigma4, 0)
    z3s[...] = pack_lanes([sigma4])
    got3 = []
    for j, dy in enumerate((1, -1)):
        got3.append(send(y3s.at[j], y3r.at[j], (0, dy, 0)))
    for j, dz in enumerate((1, -1)):
        got3.append(send(z3s, z3r.at[j], (0, 0, dz)))
    for j, (dx, lo) in enumerate(((1, X - 2), (-1, 0))):
        got3.append(send(out_sig_ref.at[lo:lo + 2], x3r.at[j], (dx, 0, 0)))
    for copy in got3:
        copy.wait_recv()
    y3 = unpack_rows(y3r[1], y3r[0])
    zpk = merge_lanes(z3r[1], z3r[0])
    z3 = jnp.concatenate([unpack_lanes(zpk, p)[None] for p in range(X)], axis=0)
    x3 = jnp.concatenate([x3r[0], sigma4, x3r[1]], axis=0)
    energy = base[4]
    for d in range(3):
        st = x_stencil(x3) if d == 0 else ring_stencil(sigma4, y3 if d == 1 else z3, d)
        ls, rs = faces(st)
        lv, rv = speed[d]
        adv_ref[1 + d] = base[1 + d] - (0.5 * STEP_DT) * difference(ls + rs, d)
        energy = energy - (0.5 * STEP_DT) * difference(ls * lv + rs * rv, d)
    adv_ref[4] = energy
    for copy in sent:
        copy.wait_send()


def solution(mesh):
    sizes = tuple(mesh.shape[a] for a in AXES)

    def on_device(conserved, sigma_guess):
        X, R, L = sigma_guess.shape
        G = X // 4
        f32 = jnp.float32
        vm = lambda *shape: pltpu.VMEM(shape, f32)
        nz, nd = len(Z_MOVES), len(XY_MOVES)
        messages = 48
        return pl.pallas_call(
            functools.partial(kernel, sizes),
            out_shape=(pltpu.VMEM(conserved.shape, f32), pltpu.VMEM(sigma_guess.shape, f32)),
            in_specs=[pl.BlockSpec(memory_space=pl.ANY)] * 2,
            out_specs=(pl.BlockSpec(memory_space=pltpu.VMEM),) * 2,
            scratch_shapes=[
                vm(*conserved.shape), vm(X, R, L),
                vm(2, 6, G, R, L), vm(2, R, L), vm(nd, R, L),
                vm(2, 5, 2, R, L), vm(2, 2, R, L), vm(2, 6, G, R, L), vm(nz, 2, R, L), vm(nd, R, L),
                vm(X, R, L), vm(2, G, R, L), vm(R, L),
                vm(2, 2, R, L), vm(2, G, R, L), vm(nz, R, L), vm(nd, R, L),
                vm(2, G, R, L), vm(R, L),
                vm(2, 2, R, L), vm(2, G, R, L), vm(2, R, L),
                pltpu.SemaphoreType.DMA((2,)),
                pltpu.SemaphoreType.DMA((messages,)),
                pltpu.SemaphoreType.DMA((messages,)),
            ],
            compiler_params=pltpu.CompilerParams(collective_id=0, has_side_effects=True),
        )(conserved, sigma_guess)

    specs = (P(None, "gx", "gy", "gz"), P("gx", "gy", "gz"))
    return jax.shard_map(on_device, mesh=mesh, in_specs=specs, out_specs=specs, check_vma=False)
```

```python
import functools
import itertools

import jax
import jax.numpy as jnp
from jax import lax
from jax.experimental import pallas as pl
from jax.experimental.pallas import tpu as pltpu
from jax.sharding import PartitionSpec as P

SWEEPS = 4
ALPHA = 10.0
GAMMA = 1.4
LAMBDA = 3.0
STEP_DT = 0.4
MESH = pl.DeviceIdType.MESH
AXES = ("gx", "gy", "gz")

OFFSETS = [o for o in itertools.product((-1, 0, 1), repeat=3) if 1 <= sum(abs(v) for v in o) <= 2]
NEAR = [o for o in OFFSETS if sum(abs(v) for v in o) == 1]
Z_MOVES = [o for o in OFFSETS if o[2] != 0]
XY_MOVES = [o for o in OFFSETS if o[0] != 0 and o[1] != 0]


def neg(offset):
    return tuple(-v for v in offset)


def iota(shape, dim):
    return lax.broadcasted_iota(jnp.int32, shape, dim)


def roll(value, shift, axis):
    size = value.shape[axis]
    shift = shift % size
    return value if shift == 0 else pltpu.roll(value, shift, axis)


def ring(core, ghost, step, axis):
    size = core.shape[axis]
    a, b = roll(core, -step, axis), roll(ghost, -step, axis)
    edge = iota(core.shape, axis) == (size - 1 if step == 1 else 0)
    return jnp.where(edge, b, a), jnp.where(edge, a, b)


def kernel(sizes, cons_hbm, sig_hbm, adv_ref, out_sig_ref, cons, sig,
           yas, zas, xar, xsr, yar, zar,
           ybs, yrs, zrs, xbr, xer, xtr, ybr, yrr, zrr, drr,
           s1, src, y2s, z2s, x2r, x2q, y2r, z2r, d2r,
           s3, y3s, z3s, x3r, y3r, z3r, d3r,
           in_sem, send_sem, recv_sem):
    X, R, L = sig.shape
    me = [lax.axis_index(a) for a in AXES]

    def device(offset):
        return {a: lax.rem(me[i] + offset[i] + sizes[i], sizes[i]) for i, a in enumerate(AXES)}

    load_c = pltpu.make_async_copy(cons_hbm, cons, in_sem.at[0])
    load_s = pltpu.make_async_copy(sig_hbm, sig, in_sem.at[1])
    load_c.start()
    load_s.start()
    barrier = pltpu.get_barrier_semaphore()
    for o in NEAR:
        pl.semaphore_signal(barrier, inc=1, device_id=device(o), device_id_type=MESH)

    sent = []
    count = [0]

    def send(src, dst, offset):
        n = count[0]
        count[0] += 1
        copy = pltpu.make_async_remote_copy(
            src_ref=src, dst_ref=dst, send_sem=send_sem.at[n], recv_sem=recv_sem.at[n],
            device_id=device(offset), device_id_type=MESH)
        copy.start()
        sent.append(copy)
        return copy

    rows = lambda shape: iota(shape, len(shape) - 2)
    lanes = lambda shape: iota(shape, len(shape) - 1)

    def pack_rows(field, first, n):
        size = X * n // R
        out = field[0:size]
        r = rows(out.shape)
        for g in range(1, R // n):
            part = roll(field[g * size:(g + 1) * size], n * g, 1)
            out = jnp.where((r + (2 * R - first - n * g)) % R < n, part, out)
        return out

    def unpack_rows(after, before, n):
        low = rows(after.shape) < R // 2
        return jnp.concatenate(
            [jnp.where(low, roll(after, -n * g, 1), roll(before, -n * g, 1)) for g in range(R // n)], axis=0)

    lane2, row2 = lanes((R, L)), rows((R, L))

    def pack_lanes(fields, width):
        out = jnp.zeros((R, L), jnp.float32)
        for k, tile in enumerate(f[p] for f in fields for p in range(X)):
            out = jnp.where(((lane2 + width // 2) % L) // width == k, roll(tile, width * k, 1), out)
        return out

    def merge_lanes(after, before, width):
        return jnp.where(lanes(after.shape) % width < width // 2, after, before)

    def unpack_lanes(packed, ks, width):
        return jnp.concatenate([roll(packed, -width * k, 1)[None] for k in ks], axis=0)

    def cat(*parts):
        return jnp.concatenate(parts, axis=0)

    def wait(copies):
        for copy in copies:
            copy.wait_recv()

    ups = ((0, 1), (1, -1))

    def edge(d, count, back=0):
        return pl.ds(X - count - back, count) if d == 1 else pl.ds(back, count)

    def send_z(src_ref, dst_ref):
        return [send(src_ref, dst_ref.at[n], o) for n, o in enumerate(Z_MOVES)]

    def z_tiles(buf, e, width, f=0):
        def of(dx, dy):
            return merge_lanes(buf[Z_MOVES.index((-dx, -dy, -1))], buf[Z_MOVES.index((-dx, -dy, 1))], width)
        k = f * X
        z = cat(unpack_lanes(of(-1, 0), range(k + X - e, k + X), width),
                unpack_lanes(of(0, 0), range(k, k + X), width),
                unpack_lanes(of(1, 0), range(k, k + e), width))
        diag = jnp.where(row2 < R // 2, of(0, 1), of(0, -1))
        return z, unpack_lanes(diag, range(k, k + X), width)

    def corners(buf, dx):
        after, before = buf[XY_MOVES.index((-dx, -1, 0))], buf[XY_MOVES.index((-dx, 1, 0))]
        return jnp.where(rows(after.shape) < R // 2, after, before)

    load_c.wait()
    load_s.wait()
    pl.semaphore_wait(barrier, len(NEAR))
    got1 = []
    state = [cons[f] for f in range(4)] + [sig[...]]
    for f in range(5):
        yas[0, f] = pack_rows(state[f], R - 1, 1)
        yas[1, f] = pack_rows(state[f], 0, 1)
    for j, d in ups:
        got1.append(send(yas.at[j], yar.at[j], (0, d, 0)))
    for j, d in ups:
        got1.append(send(cons.at[0:4, edge(d, 1)], xar.at[j], (d, 0, 0)))
        got1.append(send(sig.at[edge(d, 1)], xsr.at[j], (d, 0, 0)))
    energy = cons[4]
    zas[0] = pack_lanes(state[0:4], 4)
    zas[1] = pack_lanes([state[4], energy], 4)
    for j, d in ups:
        got1.append(send(zas, zar.at[j], (0, 0, d)))

    late, late_rho = [], []
    for f in range(4):
        field = state[1 + f] if f < 3 else energy
        ybs[0, f] = pack_rows(field, R - 2, 2)
        ybs[1, f] = pack_rows(field, 0, 2)
    yrs[0] = pack_rows(state[0], R // 2, R // 2)
    yrs[1] = pack_rows(state[0], 0, R // 2)
    for j, d in ups:
        late.append(send(yrs.at[j], yrr.at[j], (0, d, 0)))
        late.append(send(ybs.at[j], ybr.at[j], (0, d, 0)))
        late.append(send(cons.at[0:5, edge(d, 1, 1)], xbr.at[j], (d, 0, 0)))
        late.append(send(cons.at[4, edge(d, 1)], xer.at[j], (d, 0, 0)))
        late_rho.append(send(cons.at[0, edge(d, 1, 2)], xtr.at[j], (d, 0, 0)))
    zrs[...] = pack_lanes([state[0]], 8)

    wait(got1)
    late_rho += [send(cons.at[0, edge(o[0], 2)], drr.at[n], o) for n, o in enumerate(XY_MOVES)]
    late_rho += send_z(zrs, zrr)

    zmerged = [merge_lanes(zar[1, v], zar[0, v], 4) for v in range(2)]

    def near(f):
        ghost_x = (xar[0, f], xar[1, f]) if f < 4 else (xsr[0], xsr[1])
        y = unpack_rows(yar[1, f], yar[0, f], 1)
        z = unpack_lanes(zmerged[f // 4], [(f % 4) * X + p for p in range(X)], 4)
        return cat(ghost_x[0], state[f], ghost_x[1]), y, z

    def neighbours(field):
        c, y, z = field
        m = c[1:X + 1]
        return [(c[2:X + 2], c[0:X]),
                (ring(m, y, 1, 1)[0], ring(m, y, -1, 1)[0]),
                (ring(m, z, 1, 2)[0], ring(m, z, -1, 2)[0])]

    def coefficients(inv_m, inv_n):
        ws = [[0.5 * (inv_m + inv_n[d][s]) for s in range(2)] for d in range(3)]
        return ws, ALPHA / (inv_m + ALPHA * sum(w for pair in ws for w in pair))

    def update(source, ws, scale, nbr):
        acc = source
        for d in range(3):
            for s in range(2):
                acc = acc + ws[d][s] * nbr[d][s]
        return acc * scale

    ext = [near(f) for f in range(5)]
    inv = tuple(1.0 / v for v in ext[0])
    g = []
    for k in (1, 2, 3):
        n = neighbours(tuple(m * r for m, r in zip(ext[k], inv)))
        g.append([0.5 * (n[d][0] - n[d][1]) for d in range(3)])
    div = g[0][0] + g[1][1] + g[2][2]
    source = (g[0][0] * g[0][0] + g[1][1] * g[1][1] + g[2][2] * g[2][2]
              + 2.0 * (g[0][1] * g[1][0] + g[0][2] * g[2][0] + g[1][2] * g[2][1]) + div * div)
    src[...] = source
    near_w, near_scale = coefficients(inv[0][1:X + 1], neighbours(inv))
    sigma1 = update(source, near_w, near_scale, neighbours(ext[4]))

    s1[...] = sigma1
    for j, first in ((0, R - 2), (1, 0)):
        y2s[j, 0] = pack_rows(sigma1, first, 2)
        y2s[j, 1] = pack_rows(source, first, 2)
    z2s[...] = pack_lanes([sigma1, source], 4)
    got2 = [send(s1.at[X - 1 if o[0] == 1 else 0], d2r.at[n], o) for n, o in enumerate(XY_MOVES)]
    got2 += send_z(z2s, z2r)
    for j, d in ups:
        got2.append(send(y2s.at[j], y2r.at[j], (0, d, 0)))
        got2.append(send(s1.at[edge(d, 2)], x2r.at[j], (d, 0, 0)))
        got2.append(send(src.at[edge(d, 2)], x2q.at[j], (d, 0, 0)))

    wait(late)
    core = state[0:4] + [energy]
    rho_y = unpack_rows(yrr[1], yrr[0], R // 2)
    xc = [cat(xbr[0, f], xar[0, f], core[f], xar[1, f], xbr[1, f]) for f in range(4)]
    xc.append(cat(xbr[0, 4], xer[0], energy, xer[1], xbr[1, 4]))
    yc = [rho_y] + [unpack_rows(ybr[1, f], ybr[0, f], 2) for f in range(4)]
    zc = [ext[f][2] for f in range(4)] + [unpack_lanes(zmerged[1], range(X, 2 * X), 4)]

    def x_stencil(c):
        return c[0:X + 1], c[1:X + 2], c[2:X + 3], c[3:X + 4]

    def ring_stencil(c, gh, axis):
        m, p = ring(c, gh, -1, axis), ring(c, gh, 1, axis)
        return cat(*m), cat(c, gh), cat(*p), cat(*ring(p[0], p[1], 1, axis))

    def faces(st):
        m, q, p, pp = st
        sixth = 1.0 / 6.0
        return (5.0 * q + 2.0 * p - m) * sixth, (2.0 * q + 5.0 * p - pp) * sixth

    def plain_flux(s, d):
        r = 1.0 / s[0]
        v = s[1 + d] * r
        pressure = (GAMMA - 1.0) * (s[4] - 0.5 * (s[1] * s[1] + s[2] * s[2] + s[3] * s[3]) * r)
        out = [s[1 + d]]
        for k in range(3):
            out.append(s[1 + k] * v + pressure if k == d else s[1 + k] * v)
        out.append((s[4] + pressure) * v)
        return out, v

    def difference(flux, d):
        if d == 0:
            return flux[1:X + 1] - flux[0:X]
        return flux[0:X] - ring(flux[0:X], flux[X:2 * X], -1, d)[0]

    base = [None] * 5
    speed = []
    for d in range(3):
        if d == 0:
            lr = [faces(x_stencil(c)) for c in xc]
        else:
            lr = [faces(ring_stencil(c, gh, d)) for c, gh in zip(core, (None, yc, zc)[d])]
        lf, lv = plain_flux([v[0] for v in lr], d)
        rf, rv = plain_flux([v[1] for v in lr], d)
        speed.append((lv, rv))
        for k in range(5):
            flux = 0.5 * (lf[k] + rf[k]) - (0.5 * LAMBDA) * (lr[k][1] - lr[k][0])
            change = difference(flux, d)
            base[k] = change if base[k] is None else base[k] + change
    base = [core[k] - STEP_DT * base[k] for k in range(5)]
    adv_ref[0] = base[0]

    def around(field, e):
        c, y, z, w = field
        size = X + 2 * e
        cm = c[1:size + 1]
        own = slice(e, e + X)
        yp, ym = ring(cm, y, 1, 1), ring(cm, y, -1, 1)
        zp, zm = ring(cm, z, 1, 2), ring(cm, z, -1, 2)
        zy = [ring(z[own], w, s, 1)[0] for s in (1, -1)]
        yz = [ring(y[own], w, s, 2)[0] for s in (1, -1)]
        xs = lambda t: (t[e + 1:e + X + 1], t[e - 1:e + X - 1])
        return ([(c[2:size + 2], c[0:size]), (yp[0], ym[0]), (zp[0], zm[0])],
                [xs(y), (yp[1][own], ym[1][own]), yz],
                [xs(z), zy, (zp[1][own], zm[1][own])])

    wait(late_rho)
    rho_c = cat(xtr[0], xc[0], xtr[1])
    rho_z, rho_w = z_tiles(zrr, 2, 8)
    inv = tuple(1.0 / v for v in (rho_c, cat(corners(drr, -1), rho_y, corners(drr, 1)), rho_z, rho_w))
    inv_n = around(inv, 2)
    inv_m = (inv[0][1:X + 5], inv[1][2:X + 2], inv[2][2:X + 2])
    coef = [coefficients(m, n) for m, n in zip(inv_m, inv_n)]

    wait(got2)
    z, w = z_tiles(z2r, 1, 4)
    field = (cat(x2r[0], sigma1, x2r[1]),
             cat(corners(d2r, -1)[None], unpack_rows(y2r[1, 0], y2r[0, 0], 2), corners(d2r, 1)[None]), z, w)
    zs = merge_lanes(z2r[Z_MOVES.index((0, 0, -1))], z2r[Z_MOVES.index((0, 0, 1))], 4)
    sources = (cat(x2q[0], source, x2q[1]), unpack_rows(y2r[1, 1], y2r[0, 1], 2),
               unpack_lanes(zs, range(X, 2 * X), 4))
    inner = slice(1, X + 3)
    n = around(field, 1)
    c = update(sources[0][inner], [[v[inner] for v in pair] for pair in coef[0][0]], coef[0][1][inner], n[0])
    y = update(sources[1], *coef[1], n[1])
    z = update(sources[2], *coef[2], n[2])
    sigma3 = update(source, near_w, near_scale, neighbours((c, y, z)))

    s3[...] = sigma3
    y3s[0] = pack_rows(sigma3, R // 2, R // 2)
    y3s[1] = pack_rows(sigma3, 0, R // 2)
    z3s[...] = pack_lanes([sigma3], 8)
    got3 = [send(s3.at[edge(o[0], 2)], d3r.at[k], o) for k, o in enumerate(XY_MOVES)]
    got3 += send_z(z3s, z3r)
    for j, d in ups:
        got3.append(send(y3s.at[j], y3r.at[j], (0, d, 0)))
        got3.append(send(s3.at[edge(d, 3)], x3r.at[j], (d, 0, 0)))
    wait(got3)

    z, w = z_tiles(z3r, 2, 8)
    field = (cat(x3r[0], sigma3, x3r[1]),
             cat(corners(d3r, -1), unpack_rows(y3r[1], y3r[0], R // 2), corners(d3r, 1)), z, w)
    n = around(field, 2)
    c, y, z = (update(sources[t], *coef[t], n[t]) for t in range(3))
    sigma4 = c[2:X + 2]
    out_sig_ref[...] = sigma4
    total = base[4]
    for d in range(3):
        ls, rs = faces(x_stencil(c) if d == 0 else ring_stencil(sigma4, y if d == 1 else z, d))
        lv, rv = speed[d]
        adv_ref[1 + d] = base[1 + d] - (0.5 * STEP_DT) * difference(ls + rs, d)
        total = total - (0.5 * STEP_DT) * difference(ls * lv + rs * rv, d)
    adv_ref[4] = total
    for copy in sent:
        copy.wait_send()


def solution(mesh):
    sizes = tuple(mesh.shape[a] for a in AXES)

    def on_device(conserved, sigma_guess):
        X, R, L = sigma_guess.shape
        A, B, H = X // R, 2 * X // R, X // 2
        f32 = jnp.float32
        vm = lambda *shape: pltpu.VMEM(shape, f32)
        nz, nd = len(Z_MOVES), len(XY_MOVES)
        messages = 80
        return pl.pallas_call(
            functools.partial(kernel, sizes),
            out_shape=(pltpu.VMEM(conserved.shape, f32), pltpu.VMEM(sigma_guess.shape, f32)),
            in_specs=[pl.BlockSpec(memory_space=pl.ANY)] * 2,
            out_specs=(pl.BlockSpec(memory_space=pltpu.VMEM),) * 2,
            scratch_shapes=[
                vm(*conserved.shape), vm(X, R, L),
                vm(2, 5, A, R, L), vm(2, R, L), vm(2, 4, 1, R, L), vm(2, 1, R, L), vm(2, 5, A, R, L), vm(2, 2, R, L),
                vm(2, 4, B, R, L), vm(2, H, R, L), vm(R, L), vm(2, 5, 1, R, L), vm(2, 1, R, L), vm(2, 1, R, L),
                vm(2, 4, B, R, L), vm(2, H, R, L), vm(nz, R, L), vm(nd, 2, R, L),
                vm(X, R, L), vm(X, R, L), vm(2, 2, B, R, L), vm(R, L),
                vm(2, 2, R, L), vm(2, 2, R, L), vm(2, 2, B, R, L), vm(nz, R, L), vm(nd, R, L),
                vm(X, R, L), vm(2, H, R, L), vm(R, L),
                vm(2, 3, R, L), vm(2, H, R, L), vm(nz, R, L), vm(nd, 2, R, L),
                pltpu.SemaphoreType.DMA((2,)),
                pltpu.SemaphoreType.DMA((messages,)),
                pltpu.SemaphoreType.DMA((messages,)),
            ],
            compiler_params=pltpu.CompilerParams(collective_id=0, has_side_effects=True),
        )(conserved, sigma_guess)

    specs = (P(None, "gx", "gy", "gz"), P("gx", "gy", "gz"))
    return jax.shard_map(on_device, mesh=mesh, in_specs=specs, out_specs=specs, check_vma=False)
```

```python
import functools
import itertools

import jax
import jax.numpy as jnp
from jax import lax
from jax.experimental import pallas as pl
from jax.experimental.pallas import tpu as pltpu
from jax.sharding import PartitionSpec as P

SWEEPS = 4
ALPHA = 10.0
GAMMA = 1.4
LAMBDA = 3.0
STEP_DT = 0.4
MESH = pl.DeviceIdType.MESH
AXES = ("gx", "gy", "gz")

OFFSETS = [o for o in itertools.product((-1, 0, 1), repeat=3) if 1 <= sum(abs(v) for v in o) <= 2]
NEAR = [o for o in OFFSETS if sum(abs(v) for v in o) == 1]
Z_MOVES = [o for o in OFFSETS if o[2] != 0]
XY_MOVES = [o for o in OFFSETS if o[0] != 0 and o[1] != 0]


def neg(offset):
    return tuple(-v for v in offset)


def iota(shape, dim):
    return lax.broadcasted_iota(jnp.int32, shape, dim)


def roll(value, shift, axis):
    size = value.shape[axis]
    shift = shift % size
    return value if shift == 0 else pltpu.roll(value, shift, axis)


def ring(core, ghost, step, axis):
    size = core.shape[axis]
    a, b = roll(core, -step, axis), roll(ghost, -step, axis)
    edge = iota(core.shape, axis) == (size - 1 if step == 1 else 0)
    return jnp.where(edge, b, a), jnp.where(edge, a, b)


def kernel(sizes, cons_hbm, sig_hbm, adv_ref, out_sig_ref, cons, sig,
           yas, zas, xar, xsr, yar, zar,
           ybs, yrs, zrs, xbr, xer, xtr, ybr, yrr, zrr, drr,
           s1, src, y2s, z2s, x2r, x2q, y2r, z2r, d2r,
           s3, y3s, z3s, x3r, y3r, z3r, d3r,
           in_sem, send_sem, recv_sem):
    X, R, L = sig.shape
    me = [lax.axis_index(a) for a in AXES]

    def device(offset):
        return {a: lax.rem(me[i] + offset[i] + sizes[i], sizes[i]) for i, a in enumerate(AXES)}

    load_c = pltpu.make_async_copy(cons_hbm, cons, in_sem.at[0])
    load_s = pltpu.make_async_copy(sig_hbm, sig, in_sem.at[1])
    load_c.start()
    load_s.start()
    barrier = pltpu.get_barrier_semaphore()
    for o in NEAR:
        pl.semaphore_signal(barrier, inc=1, device_id=device(o), device_id_type=MESH)

    sent = []
    count = [0]

    def send(src, dst, offset):
        n = count[0]
        count[0] += 1
        copy = pltpu.make_async_remote_copy(
            src_ref=src, dst_ref=dst, send_sem=send_sem.at[n], recv_sem=recv_sem.at[n],
            device_id=device(offset), device_id_type=MESH)
        copy.start()
        sent.append(copy)
        return copy

    rows = lambda shape: iota(shape, len(shape) - 2)
    lanes = lambda shape: iota(shape, len(shape) - 1)

    def pack_rows(field, first, n):
        size = X * n // R
        out = field[0:size]
        r = rows(out.shape)
        for g in range(1, R // n):
            part = roll(field[g * size:(g + 1) * size], n * g, 1)
            out = jnp.where((r + (2 * R - first - n * g)) % R < n, part, out)
        return out

    def unpack_rows(after, before, n):
        low = rows(after.shape) < R // 2
        return jnp.concatenate(
            [jnp.where(low, roll(after, -n * g, 1), roll(before, -n * g, 1)) for g in range(R // n)], axis=0)

    lane2, row2 = lanes((R, L)), rows((R, L))

    def pack_lanes(fields, width):
        out = jnp.zeros((R, L), jnp.float32)
        for k, tile in enumerate(f[p] for f in fields for p in range(X)):
            out = jnp.where(((lane2 + width // 2) % L) // width == k, roll(tile, width * k, 1), out)
        return out

    def merge_lanes(after, before, width):
        return jnp.where(lanes(after.shape) % width < width // 2, after, before)

    def unpack_lanes(packed, ks, width):
        return jnp.concatenate([roll(packed, -width * k, 1)[None] for k in ks], axis=0)

    def cat(*parts):
        return jnp.concatenate(parts, axis=0)

    def wait(copies):
        for copy in copies:
            copy.wait_recv()

    ups = ((0, 1), (1, -1))

    def edge(d, count, back=0):
        return pl.ds(X - count - back, count) if d == 1 else pl.ds(back, count)

    def send_z(src_ref, dst_ref):
        return [send(src_ref, dst_ref.at[n], o) for n, o in enumerate(Z_MOVES)]

    def z_tiles(buf, e, width, f=0):
        def of(dx, dy):
            return merge_lanes(buf[Z_MOVES.index((-dx, -dy, -1))], buf[Z_MOVES.index((-dx, -dy, 1))], width)
        k = f * X
        z = cat(unpack_lanes(of(-1, 0), range(k + X - e, k + X), width),
                unpack_lanes(of(0, 0), range(k, k + X), width),
                unpack_lanes(of(1, 0), range(k, k + e), width))
        diag = jnp.where(row2 < R // 2, of(0, 1), of(0, -1))
        return z, unpack_lanes(diag, range(k, k + X), width)

    def corners(buf, dx):
        after, before = buf[XY_MOVES.index((-dx, -1, 0))], buf[XY_MOVES.index((-dx, 1, 0))]
        return jnp.where(rows(after.shape) < R // 2, after, before)

    load_c.wait()
    load_s.wait()
    pl.semaphore_wait(barrier, len(NEAR))
    got1 = []
    state = [cons[f] for f in range(4)] + [sig[...]]
    for f in range(5):
        yas[0, f] = pack_rows(state[f], R - 1, 1)
        yas[1, f] = pack_rows(state[f], 0, 1)
    for j, d in ups:
        got1.append(send(yas.at[j], yar.at[j], (0, d, 0)))
    for j, d in ups:
        got1.append(send(cons.at[0:4, edge(d, 1)], xar.at[j], (d, 0, 0)))
        got1.append(send(sig.at[edge(d, 1)], xsr.at[j], (d, 0, 0)))
    energy = cons[4]
    zas[0] = pack_lanes(state[0:4], 4)
    zas[1] = pack_lanes([state[4], energy], 4)
    for j, d in ups:
        got1.append(send(zas, zar.at[j], (0, 0, d)))

    late_rho = []
    yrs[0] = pack_rows(state[0], R // 2, R // 2)
    yrs[1] = pack_rows(state[0], 0, R // 2)
    for j, d in ups:
        late_rho.append(send(yrs.at[j], yrr.at[j], (0, d, 0)))
        late_rho.append(send(cons.at[0, edge(d, 2, 1)], xtr.at[j], (d, 0, 0)))
    zrs[...] = pack_lanes([state[0]], 8)

    wait(got1)
    late_rho += [send(cons.at[0, edge(o[0], 2)], drr.at[n], o) for n, o in enumerate(XY_MOVES)]
    late_rho += send_z(zrs, zrr)

    zmerged = [merge_lanes(zar[1, v], zar[0, v], 4) for v in range(2)]

    def near(f):
        ghost_x = (xar[0, f], xar[1, f]) if f < 4 else (xsr[0], xsr[1])
        y = unpack_rows(yar[1, f], yar[0, f], 1)
        z = unpack_lanes(zmerged[f // 4], [(f % 4) * X + p for p in range(X)], 4)
        return cat(ghost_x[0], state[f], ghost_x[1]), y, z

    def neighbours(field):
        c, y, z = field
        m = c[1:X + 1]
        return [(c[2:X + 2], c[0:X]),
                (ring(m, y, 1, 1)[0], ring(m, y, -1, 1)[0]),
                (ring(m, z, 1, 2)[0], ring(m, z, -1, 2)[0])]

    def coefficients(inv_m, inv_n):
        ws = [[0.5 * (inv_m + inv_n[d][s]) for s in range(2)] for d in range(3)]
        return ws, ALPHA / (inv_m + ALPHA * sum(w for pair in ws for w in pair))

    def update(source, ws, scale, nbr):
        acc = source
        for d in range(3):
            for s in range(2):
                acc = acc + ws[d][s] * nbr[d][s]
        return acc * scale

    ext = [near(f) for f in range(5)]
    inv = tuple(1.0 / v for v in ext[0])
    g = []
    for k in (1, 2, 3):
        n = neighbours(tuple(m * r for m, r in zip(ext[k], inv)))
        g.append([0.5 * (n[d][0] - n[d][1]) for d in range(3)])
    div = g[0][0] + g[1][1] + g[2][2]
    source = (g[0][0] * g[0][0] + g[1][1] * g[1][1] + g[2][2] * g[2][2]
              + 2.0 * (g[0][1] * g[1][0] + g[0][2] * g[2][0] + g[1][2] * g[2][1]) + div * div)
    src[...] = source
    near_w, near_scale = coefficients(inv[0][1:X + 1], neighbours(inv))
    sigma1 = update(source, near_w, near_scale, neighbours(ext[4]))

    s1[...] = sigma1
    for j, first in ((0, R - 2), (1, 0)):
        y2s[j, 0] = pack_rows(sigma1, first, 2)
        y2s[j, 1] = pack_rows(source, first, 2)
    z2s[...] = pack_lanes([sigma1, source], 4)
    got2 = [send(s1.at[X - 1 if o[0] == 1 else 0], d2r.at[n], o) for n, o in enumerate(XY_MOVES)]
    got2 += send_z(z2s, z2r)
    for j, d in ups:
        got2.append(send(y2s.at[j], y2r.at[j], (0, d, 0)))
        got2.append(send(s1.at[edge(d, 2)], x2r.at[j], (d, 0, 0)))
        got2.append(send(src.at[edge(d, 2)], x2q.at[j], (d, 0, 0)))

    late = []
    for f in range(4):
        part = state[1 + f] if f < 3 else energy
        ybs[0, f] = pack_rows(part, R - 2, 2)
        ybs[1, f] = pack_rows(part, 0, 2)
    for j, d in ups:
        late.append(send(ybs.at[j], ybr.at[j], (0, d, 0)))
        late.append(send(cons.at[1:5, edge(d, 1, 1)], xbr.at[j], (d, 0, 0)))
        late.append(send(cons.at[4, edge(d, 1)], xer.at[j], (d, 0, 0)))
    def around(field, e):
        c, y, z, w = field
        size = X + 2 * e
        cm = c[1:size + 1]
        own = slice(e, e + X)
        yp, ym = ring(cm, y, 1, 1), ring(cm, y, -1, 1)
        zp, zm = ring(cm, z, 1, 2), ring(cm, z, -1, 2)
        zy = [ring(z[own], w, s, 1)[0] for s in (1, -1)]
        yz = [ring(y[own], w, s, 2)[0] for s in (1, -1)]
        xs = lambda t: (t[e + 1:e + X + 1], t[e - 1:e + X - 1])
        return ([(c[2:size + 2], c[0:size]), (yp[0], ym[0]), (zp[0], zm[0])],
                [xs(y), (yp[1][own], ym[1][own]), yz],
                [xs(z), zy, (zp[1][own], zm[1][own])])

    wait(late_rho)
    rho_y = unpack_rows(yrr[1], yrr[0], R // 2)
    rho_c = cat(xtr[0], xar[0, 0], state[0], xar[1, 0], xtr[1])
    rho_z, rho_w = z_tiles(zrr, 2, 8)
    inv = tuple(1.0 / v for v in (rho_c, cat(corners(drr, -1), rho_y, corners(drr, 1)), rho_z, rho_w))
    inv_n = around(inv, 2)
    inv_m = (inv[0][1:X + 5], inv[1][2:X + 2], inv[2][2:X + 2])
    coef = [coefficients(m, n) for m, n in zip(inv_m, inv_n)]

    wait(got2)
    z, w = z_tiles(z2r, 1, 4)
    field = (cat(x2r[0], sigma1, x2r[1]),
             cat(corners(d2r, -1)[None], unpack_rows(y2r[1, 0], y2r[0, 0], 2), corners(d2r, 1)[None]), z, w)
    zs = merge_lanes(z2r[Z_MOVES.index((0, 0, -1))], z2r[Z_MOVES.index((0, 0, 1))], 4)
    sources = (cat(x2q[0], source, x2q[1]), unpack_rows(y2r[1, 1], y2r[0, 1], 2),
               unpack_lanes(zs, range(X, 2 * X), 4))
    inner = slice(1, X + 3)
    n = around(field, 1)
    c = update(sources[0][inner], [[v[inner] for v in pair] for pair in coef[0][0]], coef[0][1][inner], n[0])
    y = update(sources[1], *coef[1], n[1])
    z = update(sources[2], *coef[2], n[2])
    sigma3 = update(source, near_w, near_scale, neighbours((c, y, z)))

    s3[...] = sigma3
    y3s[0] = pack_rows(sigma3, R // 2, R // 2)
    y3s[1] = pack_rows(sigma3, 0, R // 2)
    z3s[...] = pack_lanes([sigma3], 8)
    got3 = [send(s3.at[edge(o[0], 2)], d3r.at[k], o) for k, o in enumerate(XY_MOVES)]
    got3 += send_z(z3s, z3r)
    for j, d in ups:
        got3.append(send(y3s.at[j], y3r.at[j], (0, d, 0)))
        got3.append(send(s3.at[edge(d, 3)], x3r.at[j], (d, 0, 0)))
    wait(late)
    core = state[0:4] + [energy]
    xc = [rho_c[1:X + 5]] + [cat(xbr[0, f - 1], xar[0, f], core[f], xar[1, f], xbr[1, f - 1]) for f in (1, 2, 3)]
    xc.append(cat(xbr[0, 3], xer[0], energy, xer[1], xbr[1, 3]))
    yc = [rho_y] + [unpack_rows(ybr[1, f], ybr[0, f], 2) for f in range(4)]
    zc = [ext[f][2] for f in range(4)] + [unpack_lanes(zmerged[1], range(X, 2 * X), 4)]

    def x_stencil(c):
        return c[0:X + 1], c[1:X + 2], c[2:X + 3], c[3:X + 4]

    def ring_stencil(c, gh, axis):
        m, p = ring(c, gh, -1, axis), ring(c, gh, 1, axis)
        return cat(*m), cat(c, gh), cat(*p), cat(*ring(p[0], p[1], 1, axis))

    def faces(st):
        m, q, p, pp = st
        sixth = 1.0 / 6.0
        return (5.0 * q + 2.0 * p - m) * sixth, (2.0 * q + 5.0 * p - pp) * sixth

    def plain_flux(s, d):
        r = 1.0 / s[0]
        v = s[1 + d] * r
        pressure = (GAMMA - 1.0) * (s[4] - 0.5 * (s[1] * s[1] + s[2] * s[2] + s[3] * s[3]) * r)
        out = [s[1 + d]]
        for k in range(3):
            out.append(s[1 + k] * v + pressure if k == d else s[1 + k] * v)
        out.append((s[4] + pressure) * v)
        return out, v

    def difference(flux, d):
        if d == 0:
            return flux[1:X + 1] - flux[0:X]
        return flux[0:X] - ring(flux[0:X], flux[X:2 * X], -1, d)[0]

    base = [None] * 5
    speed = []
    for d in range(3):
        if d == 0:
            lr = [faces(x_stencil(c)) for c in xc]
        else:
            lr = [faces(ring_stencil(c, gh, d)) for c, gh in zip(core, (None, yc, zc)[d])]
        lf, lv = plain_flux([v[0] for v in lr], d)
        rf, rv = plain_flux([v[1] for v in lr], d)
        speed.append((lv, rv))
        for k in range(5):
            flux = 0.5 * (lf[k] + rf[k]) - (0.5 * LAMBDA) * (lr[k][1] - lr[k][0])
            change = difference(flux, d)
            base[k] = change if base[k] is None else base[k] + change
    base = [core[k] - STEP_DT * base[k] for k in range(5)]
    adv_ref[0] = base[0]

    wait(got3)

    z, w = z_tiles(z3r, 2, 8)
    field = (cat(x3r[0], sigma3, x3r[1]),
             cat(corners(d3r, -1), unpack_rows(y3r[1], y3r[0], R // 2), corners(d3r, 1)), z, w)
    n = around(field, 2)
    c, y, z = (update(sources[t], *coef[t], n[t]) for t in range(3))
    sigma4 = c[2:X + 2]
    out_sig_ref[...] = sigma4
    total = base[4]
    for d in range(3):
        ls, rs = faces(x_stencil(c) if d == 0 else ring_stencil(sigma4, y if d == 1 else z, d))
        lv, rv = speed[d]
        adv_ref[1 + d] = base[1 + d] - (0.5 * STEP_DT) * difference(ls + rs, d)
        total = total - (0.5 * STEP_DT) * difference(ls * lv + rs * rv, d)
    adv_ref[4] = total
    for copy in sent:
        copy.wait_send()


def solution(mesh):
    sizes = tuple(mesh.shape[a] for a in AXES)

    def on_device(conserved, sigma_guess):
        X, R, L = sigma_guess.shape
        A, B, H = X // R, 2 * X // R, X // 2
        f32 = jnp.float32
        vm = lambda *shape: pltpu.VMEM(shape, f32)
        nz, nd = len(Z_MOVES), len(XY_MOVES)
        messages = 80
        return pl.pallas_call(
            functools.partial(kernel, sizes),
            out_shape=(pltpu.VMEM(conserved.shape, f32), pltpu.VMEM(sigma_guess.shape, f32)),
            in_specs=[pl.BlockSpec(memory_space=pl.ANY)] * 2,
            out_specs=(pl.BlockSpec(memory_space=pltpu.VMEM),) * 2,
            scratch_shapes=[
                vm(*conserved.shape), vm(X, R, L),
                vm(2, 5, A, R, L), vm(2, R, L), vm(2, 4, 1, R, L), vm(2, 1, R, L), vm(2, 5, A, R, L), vm(2, 2, R, L),
                vm(2, 4, B, R, L), vm(2, H, R, L), vm(R, L), vm(2, 4, 1, R, L), vm(2, 1, R, L), vm(2, 2, R, L),
                vm(2, 4, B, R, L), vm(2, H, R, L), vm(nz, R, L), vm(nd, 2, R, L),
                vm(X, R, L), vm(X, R, L), vm(2, 2, B, R, L), vm(R, L),
                vm(2, 2, R, L), vm(2, 2, R, L), vm(2, 2, B, R, L), vm(nz, R, L), vm(nd, R, L),
                vm(X, R, L), vm(2, H, R, L), vm(R, L),
                vm(2, 3, R, L), vm(2, H, R, L), vm(nz, R, L), vm(nd, 2, R, L),
                pltpu.SemaphoreType.DMA((2,)),
                pltpu.SemaphoreType.DMA((messages,)),
                pltpu.SemaphoreType.DMA((messages,)),
            ],
            compiler_params=pltpu.CompilerParams(collective_id=0, has_side_effects=True),
        )(conserved, sigma_guess)

    specs = (P(None, "gx", "gy", "gz"), P("gx", "gy", "gz"))
    return jax.shard_map(on_device, mesh=mesh, in_specs=specs, out_specs=specs, check_vma=False)
```

```python
import functools
import itertools

import jax
import jax.numpy as jnp
from jax import lax
from jax.experimental import pallas as pl
from jax.experimental.pallas import tpu as pltpu
from jax.sharding import PartitionSpec as P

SWEEPS = 4
ALPHA = 10.0
GAMMA = 1.4
LAMBDA = 3.0
STEP_DT = 0.4
MESH = pl.DeviceIdType.MESH
AXES = ("gx", "gy", "gz")

OFFSETS = [o for o in itertools.product((-1, 0, 1), repeat=3) if 1 <= sum(abs(v) for v in o) <= 2]
NEAR = [o for o in OFFSETS if sum(abs(v) for v in o) == 1]
Z_MOVES = [o for o in OFFSETS if o[2] != 0]
XY_MOVES = [o for o in OFFSETS if o[0] != 0 and o[1] != 0]


def neg(offset):
    return tuple(-v for v in offset)


def iota(shape, dim):
    return lax.broadcasted_iota(jnp.int32, shape, dim)


def roll(value, shift, axis):
    size = value.shape[axis]
    shift = shift % size
    return value if shift == 0 else pltpu.roll(value, shift, axis)


def ring(core, ghost, step, axis):
    size = core.shape[axis]
    a, b = roll(core, -step, axis), roll(ghost, -step, axis)
    edge = iota(core.shape, axis) == (size - 1 if step == 1 else 0)
    return jnp.where(edge, b, a), jnp.where(edge, a, b)


def kernel(sizes, cons_hbm, sig_hbm, adv_ref, out_sig_ref, cons, sig,
           yas, zas, xar, xsr, yar, zar,
           ybs, yrs, zrs, xbr, xer, xtr, ybr, yrr, zrr, drr,
           s1, src, y2s, z2s, x2r, x2q, y2r, z2r, d2r,
           s3, y3s, z3s, x3r, y3r, z3r, d3r,
           in_sem, send_sem, recv_sem):
    X, R, L = sig.shape
    me = [lax.axis_index(a) for a in AXES]

    def device(offset):
        return {a: lax.rem(me[i] + offset[i] + sizes[i], sizes[i]) for i, a in enumerate(AXES)}

    load_c = pltpu.make_async_copy(cons_hbm, cons, in_sem.at[0])
    load_s = pltpu.make_async_copy(sig_hbm, sig, in_sem.at[1])
    load_c.start()
    load_s.start()
    barrier = pltpu.get_barrier_semaphore()
    for o in NEAR:
        pl.semaphore_signal(barrier, inc=1, device_id=device(o), device_id_type=MESH)

    sent = []
    count = [0]

    def send(src, dst, offset):
        n = count[0]
        count[0] += 1
        copy = pltpu.make_async_remote_copy(
            src_ref=src, dst_ref=dst, send_sem=send_sem.at[n], recv_sem=recv_sem.at[n],
            device_id=device(offset), device_id_type=MESH)
        copy.start()
        sent.append(copy)
        return copy

    rows = lambda shape: iota(shape, len(shape) - 2)
    lanes = lambda shape: iota(shape, len(shape) - 1)

    def pack_rows(field, first, n):
        size = X * n // R
        out = field[0:size]
        r = rows(out.shape)
        for g in range(1, R // n):
            part = roll(field[g * size:(g + 1) * size], n * g, 1)
            out = jnp.where((r + (2 * R - first - n * g)) % R < n, part, out)
        return out

    def unpack_rows(after, before, n):
        low = rows(after.shape) < R // 2
        return jnp.concatenate(
            [jnp.where(low, roll(after, -n * g, 1), roll(before, -n * g, 1)) for g in range(R // n)], axis=0)

    lane2, row2 = lanes((R, L)), rows((R, L))

    def pack_lanes(fields, width):
        out = jnp.zeros((R, L), jnp.float32)
        for k, tile in enumerate(f[p] for f in fields for p in range(X)):
            out = jnp.where(((lane2 + width // 2) % L) // width == k, roll(tile, width * k, 1), out)
        return out

    def merge_lanes(after, before, width):
        return jnp.where(lanes(after.shape) % width < width // 2, after, before)

    def unpack_lanes(packed, ks, width):
        return jnp.concatenate([roll(packed, -width * k, 1)[None] for k in ks], axis=0)

    def cat(*parts):
        return jnp.concatenate(parts, axis=0)

    def wait(copies):
        for copy in copies:
            copy.wait_recv()

    ups = ((0, 1), (1, -1))

    def edge(d, count, back=0):
        return pl.ds(X - count - back, count) if d == 1 else pl.ds(back, count)

    def send_z(src_ref, dst_ref):
        far = [n for n, o in enumerate(Z_MOVES) if o[1]] + [n for n, o in enumerate(Z_MOVES) if o[0]]
        face = [n for n, o in enumerate(Z_MOVES) if o in NEAR]
        return ([send(src_ref, dst_ref.at[n], Z_MOVES[n]) for n in far],
                [send(src_ref, dst_ref.at[n], Z_MOVES[n]) for n in face])

    def z_face(buf, width, f=0):
        merged = merge_lanes(buf[Z_MOVES.index((0, 0, -1))], buf[Z_MOVES.index((0, 0, 1))], width)
        return unpack_lanes(merged, range(f * X, f * X + X), width)

    def z_tiles(buf, e, width, f=0):
        def of(dx, dy):
            return merge_lanes(buf[Z_MOVES.index((-dx, -dy, -1))], buf[Z_MOVES.index((-dx, -dy, 1))], width)
        k = f * X
        z = cat(unpack_lanes(of(-1, 0), range(k + X - e, k + X), width),
                unpack_lanes(of(0, 0), range(k, k + X), width),
                unpack_lanes(of(1, 0), range(k, k + e), width))
        diag = jnp.where(row2 < R // 2, of(0, 1), of(0, -1))
        return z, unpack_lanes(diag, range(k, k + X), width)

    def corners(buf, dx):
        after, before = buf[XY_MOVES.index((-dx, -1, 0))], buf[XY_MOVES.index((-dx, 1, 0))]
        return jnp.where(rows(after.shape) < R // 2, after, before)

    load_c.wait()
    load_s.wait()
    pl.semaphore_wait(barrier, len(NEAR))
    got1 = []
    state = [cons[f] for f in range(4)] + [sig[...]]
    for f in range(5):
        yas[0, f] = pack_rows(state[f], R - 1, 1)
        yas[1, f] = pack_rows(state[f], 0, 1)
    for j, d in ups:
        got1.append(send(yas.at[j], yar.at[j], (0, d, 0)))
    for j, d in ups:
        got1.append(send(cons.at[0:4, edge(d, 1)], xar.at[j], (d, 0, 0)))
        got1.append(send(sig.at[edge(d, 1)], xsr.at[j], (d, 0, 0)))
    energy = cons[4]
    zas[0] = pack_lanes(state[0:4], 4)
    zas[1] = pack_lanes([state[4], energy], 4)
    for j, d in ups:
        got1.append(send(zas, zar.at[j], (0, 0, d)))

    late_rho = []
    yrs[0] = pack_rows(state[0], R // 2, R // 2)
    yrs[1] = pack_rows(state[0], 0, R // 2)
    for j, d in ups:
        late_rho.append(send(yrs.at[j], yrr.at[j], (0, d, 0)))
        late_rho.append(send(cons.at[0, edge(d, 2, 1)], xtr.at[j], (d, 0, 0)))
    zrs[...] = pack_lanes([state[0]], 8)

    wait(got1)
    late_rho += [send(cons.at[0, edge(o[0], 2)], drr.at[n], o) for n, o in enumerate(XY_MOVES)]
    late_rho += sum(send_z(zrs, zrr), [])

    zmerged = [merge_lanes(zar[1, v], zar[0, v], 4) for v in range(2)]

    def near(f):
        ghost_x = (xar[0, f], xar[1, f]) if f < 4 else (xsr[0], xsr[1])
        y = unpack_rows(yar[1, f], yar[0, f], 1)
        z = unpack_lanes(zmerged[f // 4], [(f % 4) * X + p for p in range(X)], 4)
        return cat(ghost_x[0], state[f], ghost_x[1]), y, z

    def neighbours(field):
        c, y, z = field
        m = c[1:X + 1]
        return [(c[2:X + 2], c[0:X]),
                (ring(m, y, 1, 1)[0], ring(m, y, -1, 1)[0]),
                (ring(m, z, 1, 2)[0], ring(m, z, -1, 2)[0])]

    def coefficients(inv_m, inv_n):
        ws = [[0.5 * (inv_m + inv_n[d][s]) for s in range(2)] for d in range(3)]
        return ws, ALPHA / (inv_m + ALPHA * sum(w for pair in ws for w in pair))

    def update(source, ws, scale, nbr):
        acc = source
        for d in range(3):
            for s in range(2):
                acc = acc + ws[d][s] * nbr[d][s]
        return acc * scale

    ext = [near(f) for f in range(5)]
    inv = tuple(1.0 / v for v in ext[0])
    g = []
    for k in (1, 2, 3):
        n = neighbours(tuple(m * r for m, r in zip(ext[k], inv)))
        g.append([0.5 * (n[d][0] - n[d][1]) for d in range(3)])
    div = g[0][0] + g[1][1] + g[2][2]
    source = (g[0][0] * g[0][0] + g[1][1] * g[1][1] + g[2][2] * g[2][2]
              + 2.0 * (g[0][1] * g[1][0] + g[0][2] * g[2][0] + g[1][2] * g[2][1]) + div * div)
    src[...] = source
    near_w, near_scale = coefficients(inv[0][1:X + 1], neighbours(inv))
    sigma1 = update(source, near_w, near_scale, neighbours(ext[4]))

    s1[...] = sigma1
    far2 = [send(s1.at[X - 1 if o[0] == 1 else 0], d2r.at[n], o) for n, o in enumerate(XY_MOVES)]
    z2s[...] = pack_lanes([sigma1, source], 4)
    far, face2 = send_z(z2s, z2r)
    far2 += far
    for j, first in ((0, R - 2), (1, 0)):
        y2s[j, 0] = pack_rows(sigma1, first, 2)
        y2s[j, 1] = pack_rows(source, first, 2)
    for j, d in ups:
        face2.append(send(y2s.at[j], y2r.at[j], (0, d, 0)))
        face2.append(send(s1.at[edge(d, 2)], x2r.at[j], (d, 0, 0)))
        face2.append(send(src.at[edge(d, 2)], x2q.at[j], (d, 0, 0)))

    late = []
    for f in range(4):
        part = state[1 + f] if f < 3 else energy
        ybs[0, f] = pack_rows(part, R - 2, 2)
        ybs[1, f] = pack_rows(part, 0, 2)
    for j, d in ups:
        late.append(send(ybs.at[j], ybr.at[j], (0, d, 0)))
        late.append(send(cons.at[1:5, edge(d, 1, 1)], xbr.at[j], (d, 0, 0)))
        late.append(send(cons.at[4, edge(d, 1)], xer.at[j], (d, 0, 0)))
    def around(field, e):
        c, y, z, w = field
        own = slice(e, e + X)
        sides = lambda t, at: cat(t[at:at + e], t[X + e + at:X + 2 * e + at])
        core, cg, yg, zg = c[e + 1:e + X + 1], sides(c, 1), sides(y, 0), sides(z, 0)
        both = lambda a, b, axis, part: [ring(a, b, s, axis)[part] for s in (1, -1)]
        xs = lambda t: (t[e + 1:e + X + 1], t[e - 1:e + X - 1])
        return ([(sides(c, 2), sides(c, 0)), both(cg, yg, 1, 0), both(cg, zg, 2, 0)],
                [xs(y), both(core, y[own], 1, 1), both(y[own], w, 2, 0)],
                [xs(z), both(z[own], w, 1, 0), both(core, z[own], 2, 1)])

    wait(late_rho)
    rho_y = unpack_rows(yrr[1], yrr[0], R // 2)
    rho_c = cat(xtr[0], xar[0, 0], state[0], xar[1, 0], xtr[1])
    rho_z, rho_w = z_tiles(zrr, 2, 8)
    inv = tuple(1.0 / v for v in (rho_c, cat(corners(drr, -1), rho_y, corners(drr, 1)), rho_z, rho_w))
    inv_m = (cat(inv[0][1:3], inv[0][X + 3:X + 5]), inv[1][2:X + 2], inv[2][2:X + 2])
    coef = [coefficients(m, n) for m, n in zip(inv_m, around(inv, 2))]

    wait(face2)
    y = unpack_rows(y2r[1, 0], y2r[0, 0], 2)
    z = z_face(z2r, 4)
    sources = (cat(x2q[0], x2q[1]), unpack_rows(y2r[1, 1], y2r[0, 1], 2), z_face(z2r, 4, 1))
    c = cat(x2r[0], sigma1, x2r[1])
    sigma2 = update(source, near_w, near_scale, neighbours((c[1:X + 3], y, z)))
    wait(far2)
    z, w = z_tiles(z2r, 1, 4)
    n = around((c, cat(corners(d2r, -1)[None], y, corners(d2r, 1)[None]), z, w), 1)
    mid = slice(1, 3)
    cg = update(sources[0][mid], [[v[mid] for v in pair] for pair in coef[0][0]], coef[0][1][mid], n[0])
    y = update(sources[1], *coef[1], n[1])
    z = update(sources[2], *coef[2], n[2])
    sigma3 = update(source, near_w, near_scale, neighbours((cat(cg[0:1], sigma2, cg[1:2]), y, z)))

    s3[...] = sigma3
    far3 = [send(s3.at[edge(o[0], 2)], d3r.at[k], o) for k, o in enumerate(XY_MOVES)]
    z3s[...] = pack_lanes([sigma3], 8)
    far, face3 = send_z(z3s, z3r)
    far3 += far
    y3s[0] = pack_rows(sigma3, R // 2, R // 2)
    y3s[1] = pack_rows(sigma3, 0, R // 2)
    for j, d in ups:
        face3.append(send(y3s.at[j], y3r.at[j], (0, d, 0)))
        face3.append(send(s3.at[edge(d, 3)], x3r.at[j], (d, 0, 0)))
    wait(late)
    core = state[0:4] + [energy]
    xc = [rho_c[1:X + 5]] + [cat(xbr[0, f - 1], xar[0, f], core[f], xar[1, f], xbr[1, f - 1]) for f in (1, 2, 3)]
    xc.append(cat(xbr[0, 3], xer[0], energy, xer[1], xbr[1, 3]))
    yc = [rho_y] + [unpack_rows(ybr[1, f], ybr[0, f], 2) for f in range(4)]
    zc = [ext[f][2] for f in range(4)] + [unpack_lanes(zmerged[1], range(X, 2 * X), 4)]

    def x_stencil(c):
        return c[0:X + 1], c[1:X + 2], c[2:X + 3], c[3:X + 4]

    def ring_stencil(c, gh, axis):
        m, p = ring(c, gh, -1, axis), ring(c, gh, 1, axis)
        return cat(*m), cat(c, gh), cat(*p), cat(*ring(p[0], p[1], 1, axis))

    def faces(st):
        m, q, p, pp = st
        sixth = 1.0 / 6.0
        return (5.0 * q + 2.0 * p - m) * sixth, (2.0 * q + 5.0 * p - pp) * sixth

    def plain_flux(s, d):
        r = 1.0 / s[0]
        v = s[1 + d] * r
        pressure = (GAMMA - 1.0) * (s[4] - 0.5 * (s[1] * s[1] + s[2] * s[2] + s[3] * s[3]) * r)
        out = [s[1 + d]]
        for k in range(3):
            out.append(s[1 + k] * v + pressure if k == d else s[1 + k] * v)
        out.append((s[4] + pressure) * v)
        return out, v

    def difference(flux, d):
        if d == 0:
            return flux[1:X + 1] - flux[0:X]
        return flux[0:X] - ring(flux[0:X], flux[X:2 * X], -1, d)[0]

    base = [None] * 5
    speed = []
    for d in range(3):
        if d == 0:
            lr = [faces(x_stencil(c)) for c in xc]
        else:
            lr = [faces(ring_stencil(c, gh, d)) for c, gh in zip(core, (None, yc, zc)[d])]
        lf, lv = plain_flux([v[0] for v in lr], d)
        rf, rv = plain_flux([v[1] for v in lr], d)
        speed.append((lv, rv))
        for k in range(5):
            flux = 0.5 * (lf[k] + rf[k]) - (0.5 * LAMBDA) * (lr[k][1] - lr[k][0])
            change = difference(flux, d)
            base[k] = change if base[k] is None else base[k] + change
    base = [core[k] - STEP_DT * base[k] for k in range(5)]
    adv_ref[0] = base[0]


    wait(face3)
    y = unpack_rows(y3r[1], y3r[0], R // 2)
    c = cat(x3r[0], sigma3, x3r[1])
    sigma4 = update(source, near_w, near_scale, neighbours((c[2:X + 4], y, z_face(z3r, 8))))
    out_sig_ref[...] = sigma4
    wait(far3)
    z, w = z_tiles(z3r, 2, 8)
    n = around((c, cat(corners(d3r, -1), y, corners(d3r, 1)), z, w), 2)
    cg, y, z = (update(sources[t], *coef[t], n[t]) for t in range(3))
    c = cat(cg[0:2], sigma4, cg[2:4])
    total = base[4]
    for d in range(3):
        ls, rs = faces(x_stencil(c) if d == 0 else ring_stencil(sigma4, y if d == 1 else z, d))
        lv, rv = speed[d]
        adv_ref[1 + d] = base[1 + d] - (0.5 * STEP_DT) * difference(ls + rs, d)
        total = total - (0.5 * STEP_DT) * difference(ls * lv + rs * rv, d)
    adv_ref[4] = total
    for copy in sent:
        copy.wait_send()


def solution(mesh):
    sizes = tuple(mesh.shape[a] for a in AXES)

    def on_device(conserved, sigma_guess):
        X, R, L = sigma_guess.shape
        A, B, H = X // R, 2 * X // R, X // 2
        f32 = jnp.float32
        vm = lambda *shape: pltpu.VMEM(shape, f32)
        nz, nd = len(Z_MOVES), len(XY_MOVES)
        messages = 80
        return pl.pallas_call(
            functools.partial(kernel, sizes),
            out_shape=(pltpu.VMEM(conserved.shape, f32), pltpu.VMEM(sigma_guess.shape, f32)),
            in_specs=[pl.BlockSpec(memory_space=pl.ANY)] * 2,
            out_specs=(pl.BlockSpec(memory_space=pltpu.VMEM),) * 2,
            scratch_shapes=[
                vm(*conserved.shape), vm(X, R, L),
                vm(2, 5, A, R, L), vm(2, R, L), vm(2, 4, 1, R, L), vm(2, 1, R, L), vm(2, 5, A, R, L), vm(2, 2, R, L),
                vm(2, 4, B, R, L), vm(2, H, R, L), vm(R, L), vm(2, 4, 1, R, L), vm(2, 1, R, L), vm(2, 2, R, L),
                vm(2, 4, B, R, L), vm(2, H, R, L), vm(nz, R, L), vm(nd, 2, R, L),
                vm(X, R, L), vm(X, R, L), vm(2, 2, B, R, L), vm(R, L),
                vm(2, 2, R, L), vm(2, 2, R, L), vm(2, 2, B, R, L), vm(nz, R, L), vm(nd, R, L),
                vm(X, R, L), vm(2, H, R, L), vm(R, L),
                vm(2, 3, R, L), vm(2, H, R, L), vm(nz, R, L), vm(nd, 2, R, L),
                pltpu.SemaphoreType.DMA((2,)),
                pltpu.SemaphoreType.DMA((messages,)),
                pltpu.SemaphoreType.DMA((messages,)),
            ],
            compiler_params=pltpu.CompilerParams(collective_id=0, has_side_effects=True),
        )(conserved, sigma_guess)

    specs = (P(None, "gx", "gy", "gz"), P("gx", "gy", "gz"))
    return jax.shard_map(on_device, mesh=mesh, in_specs=specs, out_specs=specs, check_vma=False)
```

```python
import functools
import itertools

import jax
import jax.numpy as jnp
from jax import lax
from jax.experimental import pallas as pl
from jax.experimental.pallas import tpu as pltpu
from jax.sharding import PartitionSpec as P

SWEEPS = 4
ALPHA = 10.0
GAMMA = 1.4
LAMBDA = 3.0
STEP_DT = 0.4
MESH = pl.DeviceIdType.MESH
AXES = ("gx", "gy", "gz")

OFFSETS = [o for o in itertools.product((-1, 0, 1), repeat=3) if 1 <= sum(abs(v) for v in o) <= 2]
NEAR = [o for o in OFFSETS if sum(abs(v) for v in o) == 1]
Z_MOVES = [o for o in OFFSETS if o[2] != 0]
XY_MOVES = [o for o in OFFSETS if o[0] != 0 and o[1] != 0]


def neg(offset):
    return tuple(-v for v in offset)


def iota(shape, dim):
    return lax.broadcasted_iota(jnp.int32, shape, dim)


def roll(value, shift, axis):
    size = value.shape[axis]
    shift = shift % size
    return value if shift == 0 else pltpu.roll(value, shift, axis)


def ring(core, ghost, step, axis):
    size = core.shape[axis]
    a, b = roll(core, -step, axis), roll(ghost, -step, axis)
    edge = iota(core.shape, axis) == (size - 1 if step == 1 else 0)
    return jnp.where(edge, b, a), jnp.where(edge, a, b)


def kernel(sizes, cons_hbm, sig_hbm, adv_ref, out_sig_ref, cons, sig,
           yas, zas, xar, xsr, yar, zar,
           ybs, yrs, xbr, xer, xtr, ybr, yrr,
           s1, src, y2s, z2s, d2s, x2r, x2q, y2r, z2r, d2r,
           s3, y3s, z3s, x3r, y3r, z3r, d3r,
           in_sem, send_sem, recv_sem):
    X, R, L = sig.shape
    me = [lax.axis_index(a) for a in AXES]

    def device(offset):
        return {a: lax.rem(me[i] + offset[i] + sizes[i], sizes[i]) for i, a in enumerate(AXES)}

    load_c = pltpu.make_async_copy(cons_hbm, cons, in_sem.at[0])
    load_s = pltpu.make_async_copy(sig_hbm, sig, in_sem.at[1])
    load_c.start()
    load_s.start()
    barrier = pltpu.get_barrier_semaphore()
    for o in NEAR:
        pl.semaphore_signal(barrier, inc=1, device_id=device(o), device_id_type=MESH)

    sent = []
    count = [0]

    def send(src, dst, offset):
        n = count[0]
        count[0] += 1
        copy = pltpu.make_async_remote_copy(
            src_ref=src, dst_ref=dst, send_sem=send_sem.at[n], recv_sem=recv_sem.at[n],
            device_id=device(offset), device_id_type=MESH)
        copy.start()
        sent.append(copy)
        return copy

    rows = lambda shape: iota(shape, len(shape) - 2)
    lanes = lambda shape: iota(shape, len(shape) - 1)

    def pack_rows(field, first, n):
        size = X * n // R
        out = field[0:size]
        r = rows(out.shape)
        for g in range(1, R // n):
            part = roll(field[g * size:(g + 1) * size], n * g, 1)
            out = jnp.where((r + (2 * R - first - n * g)) % R < n, part, out)
        return out

    def unpack_rows(after, before, n):
        low = rows(after.shape) < R // 2
        return jnp.concatenate(
            [jnp.where(low, roll(after, -n * g, 1), roll(before, -n * g, 1)) for g in range(R // n)], axis=0)

    lane2, row2 = lanes((R, L)), rows((R, L))

    def pack_lanes(fields, width):
        out = jnp.zeros((R, L), jnp.float32)
        for k, tile in enumerate(f[p] for f in fields for p in range(X)):
            out = jnp.where(((lane2 + width // 2) % L) // width == k, roll(tile, width * k, 1), out)
        return out

    def merge_lanes(after, before, width):
        return jnp.where(lanes(after.shape) % width < width // 2, after, before)

    def unpack_lanes(packed, ks, width):
        return jnp.concatenate([roll(packed, -width * k, 1)[None] for k in ks], axis=0)

    def cat(*parts):
        return jnp.concatenate(parts, axis=0)

    def wait(copies):
        for copy in copies:
            copy.wait_recv()

    ups = ((0, 1), (1, -1))

    def edge(d, count, back=0):
        return pl.ds(X - count - back, count) if d == 1 else pl.ds(back, count)

    def send_z(src_ref, dst_ref):
        far = [n for n, o in enumerate(Z_MOVES) if o[1]] + [n for n, o in enumerate(Z_MOVES) if o[0]]
        face = [n for n, o in enumerate(Z_MOVES) if o in NEAR]
        return ([send(src_ref, dst_ref.at[n], Z_MOVES[n]) for n in far],
                [send(src_ref, dst_ref.at[n], Z_MOVES[n]) for n in face])

    def z_face(buf, width, f=0):
        merged = merge_lanes(buf[Z_MOVES.index((0, 0, -1))], buf[Z_MOVES.index((0, 0, 1))], width)
        return unpack_lanes(merged, range(f * X, f * X + X), width)

    def z_tiles(buf, e, width, f=0):
        def of(dx, dy):
            return merge_lanes(buf[Z_MOVES.index((-dx, -dy, -1))], buf[Z_MOVES.index((-dx, -dy, 1))], width)
        k = f * X
        z = cat(unpack_lanes(of(-1, 0), range(k + X - e, k + X), width),
                unpack_lanes(of(0, 0), range(k, k + X), width),
                unpack_lanes(of(1, 0), range(k, k + e), width))
        diag = jnp.where(row2 < R // 2, of(0, 1), of(0, -1))
        return z, unpack_lanes(diag, range(k, k + X), width)

    def corners(buf, dx):
        after, before = buf[XY_MOVES.index((-dx, -1, 0))], buf[XY_MOVES.index((-dx, 1, 0))]
        return jnp.where(rows(after.shape) < R // 2, after, before)

    load_c.wait()
    load_s.wait()
    pl.semaphore_wait(barrier, len(NEAR))
    got1 = []
    state = [cons[f] for f in range(4)] + [sig[...]]
    for f in range(5):
        yas[0, f] = pack_rows(state[f], R - 1, 1)
        yas[1, f] = pack_rows(state[f], 0, 1)
    for j, d in ups:
        got1.append(send(yas.at[j], yar.at[j], (0, d, 0)))
    for j, d in ups:
        got1.append(send(cons.at[0:4, edge(d, 1)], xar.at[j], (d, 0, 0)))
        got1.append(send(sig.at[edge(d, 1)], xsr.at[j], (d, 0, 0)))
    energy = cons[4]
    zas[0] = pack_lanes(state[0:4], 4)
    zas[1] = pack_lanes([state[4], energy], 4)
    for j, d in ups:
        got1.append(send(zas, zar.at[j], (0, 0, d)))

    late_rho = []
    yrs[0] = pack_rows(state[0], R // 2, R // 2)
    yrs[1] = pack_rows(state[0], 0, R // 2)
    for j, d in ups:
        late_rho.append(send(yrs.at[j], yrr.at[j], (0, d, 0)))
        late_rho.append(send(cons.at[0, edge(d, 2, 1)], xtr.at[j], (d, 0, 0)))
    z2s[1] = pack_lanes([state[0]], 8)
    d2s[0, 1:3] = state[0][X - 2:X]
    d2s[1, 1:3] = state[0][0:2]

    wait(got1)
    zmerged = [merge_lanes(zar[1, v], zar[0, v], 4) for v in range(2)]

    def near(f):
        ghost_x = (xar[0, f], xar[1, f]) if f < 4 else (xsr[0], xsr[1])
        y = unpack_rows(yar[1, f], yar[0, f], 1)
        z = unpack_lanes(zmerged[f // 4], [(f % 4) * X + p for p in range(X)], 4)
        return cat(ghost_x[0], state[f], ghost_x[1]), y, z

    def neighbours(field):
        c, y, z = field
        m = c[1:X + 1]
        return [(c[2:X + 2], c[0:X]),
                (ring(m, y, 1, 1)[0], ring(m, y, -1, 1)[0]),
                (ring(m, z, 1, 2)[0], ring(m, z, -1, 2)[0])]

    def coefficients(inv_m, inv_n):
        ws = [[0.5 * (inv_m + inv_n[d][s]) for s in range(2)] for d in range(3)]
        return ws, ALPHA / (inv_m + ALPHA * sum(w for pair in ws for w in pair))

    def update(source, ws, scale, nbr):
        acc = source
        for d in range(3):
            for s in range(2):
                acc = acc + ws[d][s] * nbr[d][s]
        return acc * scale

    ext = [near(f) for f in range(5)]
    inv = tuple(1.0 / v for v in ext[0])
    g = []
    for k in (1, 2, 3):
        n = neighbours(tuple(m * r for m, r in zip(ext[k], inv)))
        g.append([0.5 * (n[d][0] - n[d][1]) for d in range(3)])
    div = g[0][0] + g[1][1] + g[2][2]
    source = (g[0][0] * g[0][0] + g[1][1] * g[1][1] + g[2][2] * g[2][2]
              + 2.0 * (g[0][1] * g[1][0] + g[0][2] * g[2][0] + g[1][2] * g[2][1]) + div * div)
    src[...] = source
    near_w, near_scale = coefficients(inv[0][1:X + 1], neighbours(inv))
    sigma1 = update(source, near_w, near_scale, neighbours(ext[4]))

    s1[...] = sigma1
    d2s[0, 0] = sigma1[X - 1]
    d2s[1, 0] = sigma1[0]
    far2 = [send(d2s.at[0 if o[0] == 1 else 1], d2r.at[n], o) for n, o in enumerate(XY_MOVES)]
    z2s[0] = pack_lanes([sigma1, source], 4)
    far, face2 = send_z(z2s, z2r)
    far2 += far
    for j, first in ((0, R - 2), (1, 0)):
        y2s[j, 0] = pack_rows(sigma1, first, 2)
        y2s[j, 1] = pack_rows(source, first, 2)
    for j, d in ups:
        face2.append(send(y2s.at[j], y2r.at[j], (0, d, 0)))
        face2.append(send(s1.at[edge(d, 2)], x2r.at[j], (d, 0, 0)))
        face2.append(send(src.at[edge(d, 2)], x2q.at[j], (d, 0, 0)))

    late = []
    for f in range(4):
        part = state[1 + f] if f < 3 else energy
        ybs[0, f] = pack_rows(part, R - 2, 2)
        ybs[1, f] = pack_rows(part, 0, 2)
    for j, d in ups:
        late.append(send(ybs.at[j], ybr.at[j], (0, d, 0)))
        late.append(send(cons.at[1:5, edge(d, 1, 1)], xbr.at[j], (d, 0, 0)))
        late.append(send(cons.at[4, edge(d, 1)], xer.at[j], (d, 0, 0)))
    def around(field, e):
        c, y, z, w = field
        own = slice(e, e + X)
        sides = lambda t, at: cat(t[at:at + e], t[X + e + at:X + 2 * e + at])
        core, cg, yg, zg = c[e + 1:e + X + 1], sides(c, 1), sides(y, 0), sides(z, 0)
        both = lambda a, b, axis, part: [ring(a, b, s, axis)[part] for s in (1, -1)]
        xs = lambda t: (t[e + 1:e + X + 1], t[e - 1:e + X - 1])
        return ([(sides(c, 2), sides(c, 0)), both(cg, yg, 1, 0), both(cg, zg, 2, 0)],
                [xs(y), both(core, y[own], 1, 1), both(y[own], w, 2, 0)],
                [xs(z), both(z[own], w, 1, 0), both(core, z[own], 2, 1)])

    wait(late_rho + face2)
    z_near = [z2r[n, 0] if o in NEAR else None for n, o in enumerate(Z_MOVES)]
    y = unpack_rows(y2r[1, 0], y2r[0, 0], 2)
    z = z_face(z_near, 4)
    sources = (cat(x2q[0], x2q[1]), unpack_rows(y2r[1, 1], y2r[0, 1], 2), z_face(z_near, 4, 1))
    c = cat(x2r[0], sigma1, x2r[1])
    sigma2 = update(source, near_w, near_scale, neighbours((c[1:X + 3], y, z)))
    wait(far2)
    d_rho = [d2r[n, 1:3] for n in range(len(XY_MOVES))]
    d_sig = [d2r[n, 0] for n in range(len(XY_MOVES))]
    rho_y = unpack_rows(yrr[1], yrr[0], R // 2)
    rho_c = cat(xtr[0], xar[0, 0], state[0], xar[1, 0], xtr[1])
    rho_z, rho_w = z_tiles([z2r[n, 1] for n in range(len(Z_MOVES))], 2, 8)
    inv = tuple(1.0 / v for v in (rho_c, cat(corners(d_rho, -1), rho_y, corners(d_rho, 1)), rho_z, rho_w))
    inv_m = (cat(inv[0][1:3], inv[0][X + 3:X + 5]), inv[1][2:X + 2], inv[2][2:X + 2])
    coef = [coefficients(m, n) for m, n in zip(inv_m, around(inv, 2))]

    z, w = z_tiles([z2r[n, 0] for n in range(len(Z_MOVES))], 1, 4)
    n = around((c, cat(corners(d_sig, -1)[None], y, corners(d_sig, 1)[None]), z, w), 1)
    mid = slice(1, 3)
    cg = update(sources[0][mid], [[v[mid] for v in pair] for pair in coef[0][0]], coef[0][1][mid], n[0])
    y = update(sources[1], *coef[1], n[1])
    z = update(sources[2], *coef[2], n[2])
    sigma3 = update(source, near_w, near_scale, neighbours((cat(cg[0:1], sigma2, cg[1:2]), y, z)))

    s3[...] = sigma3
    far3 = [send(s3.at[edge(o[0], 2)], d3r.at[k], o) for k, o in enumerate(XY_MOVES)]
    z3s[...] = pack_lanes([sigma3], 8)
    far, face3 = send_z(z3s, z3r)
    far3 += far
    y3s[0] = pack_rows(sigma3, R // 2, R // 2)
    y3s[1] = pack_rows(sigma3, 0, R // 2)
    for j, d in ups:
        face3.append(send(y3s.at[j], y3r.at[j], (0, d, 0)))
        face3.append(send(s3.at[edge(d, 3)], x3r.at[j], (d, 0, 0)))
    wait(late)
    core = state[0:4] + [energy]
    xc = [rho_c[1:X + 5]] + [cat(xbr[0, f - 1], xar[0, f], core[f], xar[1, f], xbr[1, f - 1]) for f in (1, 2, 3)]
    xc.append(cat(xbr[0, 3], xer[0], energy, xer[1], xbr[1, 3]))
    yc = [rho_y] + [unpack_rows(ybr[1, f], ybr[0, f], 2) for f in range(4)]
    zc = [ext[f][2] for f in range(4)] + [unpack_lanes(zmerged[1], range(X, 2 * X), 4)]

    def x_stencil(c):
        return c[0:X + 1], c[1:X + 2], c[2:X + 3], c[3:X + 4]

    def ring_stencil(c, gh, axis):
        m, p = ring(c, gh, -1, axis), ring(c, gh, 1, axis)
        return cat(*m), cat(c, gh), cat(*p), cat(*ring(p[0], p[1], 1, axis))

    def faces(st):
        m, q, p, pp = st
        sixth = 1.0 / 6.0
        return (5.0 * q + 2.0 * p - m) * sixth, (2.0 * q + 5.0 * p - pp) * sixth

    def plain_flux(s, d):
        r = 1.0 / s[0]
        v = s[1 + d] * r
        pressure = (GAMMA - 1.0) * (s[4] - 0.5 * (s[1] * s[1] + s[2] * s[2] + s[3] * s[3]) * r)
        out = [s[1 + d]]
        for k in range(3):
            out.append(s[1 + k] * v + pressure if k == d else s[1 + k] * v)
        out.append((s[4] + pressure) * v)
        return out, v

    def difference(flux, d):
        if d == 0:
            return flux[1:X + 1] - flux[0:X]
        return flux[0:X] - ring(flux[0:X], flux[X:2 * X], -1, d)[0]

    base = [None] * 5
    speed = []
    for d in range(3):
        if d == 0:
            lr = [faces(x_stencil(c)) for c in xc]
        else:
            lr = [faces(ring_stencil(c, gh, d)) for c, gh in zip(core, (None, yc, zc)[d])]
        lf, lv = plain_flux([v[0] for v in lr], d)
        rf, rv = plain_flux([v[1] for v in lr], d)
        speed.append((lv, rv))
        for k in range(5):
            flux = 0.5 * (lf[k] + rf[k]) - (0.5 * LAMBDA) * (lr[k][1] - lr[k][0])
            change = difference(flux, d)
            base[k] = change if base[k] is None else base[k] + change
    base = [core[k] - STEP_DT * base[k] for k in range(5)]
    adv_ref[0] = base[0]


    wait(face3)
    y = unpack_rows(y3r[1], y3r[0], R // 2)
    c = cat(x3r[0], sigma3, x3r[1])
    sigma4 = update(source, near_w, near_scale, neighbours((c[2:X + 4], y, z_face(z3r, 8))))
    out_sig_ref[...] = sigma4
    wait(far3)
    z, w = z_tiles(z3r, 2, 8)
    n = around((c, cat(corners(d3r, -1), y, corners(d3r, 1)), z, w), 2)
    cg, y, z = (update(sources[t], *coef[t], n[t]) for t in range(3))
    c = cat(cg[0:2], sigma4, cg[2:4])
    total = base[4]
    for d in range(3):
        ls, rs = faces(x_stencil(c) if d == 0 else ring_stencil(sigma4, y if d == 1 else z, d))
        lv, rv = speed[d]
        adv_ref[1 + d] = base[1 + d] - (0.5 * STEP_DT) * difference(ls + rs, d)
        total = total - (0.5 * STEP_DT) * difference(ls * lv + rs * rv, d)
    adv_ref[4] = total
    for copy in sent:
        copy.wait_send()


def solution(mesh):
    sizes = tuple(mesh.shape[a] for a in AXES)

    def on_device(conserved, sigma_guess):
        X, R, L = sigma_guess.shape
        A, B, H = X // R, 2 * X // R, X // 2
        f32 = jnp.float32
        vm = lambda *shape: pltpu.VMEM(shape, f32)
        nz, nd = len(Z_MOVES), len(XY_MOVES)
        messages = 80
        return pl.pallas_call(
            functools.partial(kernel, sizes),
            out_shape=(pltpu.VMEM(conserved.shape, f32), pltpu.VMEM(sigma_guess.shape, f32)),
            in_specs=[pl.BlockSpec(memory_space=pl.ANY)] * 2,
            out_specs=(pl.BlockSpec(memory_space=pltpu.VMEM),) * 2,
            scratch_shapes=[
                vm(*conserved.shape), vm(X, R, L),
                vm(2, 5, A, R, L), vm(2, R, L), vm(2, 4, 1, R, L), vm(2, 1, R, L), vm(2, 5, A, R, L), vm(2, 2, R, L),
                vm(2, 4, B, R, L), vm(2, H, R, L), vm(2, 4, 1, R, L), vm(2, 1, R, L), vm(2, 2, R, L),
                vm(2, 4, B, R, L), vm(2, H, R, L),
                vm(X, R, L), vm(X, R, L), vm(2, 2, B, R, L), vm(2, R, L), vm(2, 3, R, L),
                vm(2, 2, R, L), vm(2, 2, R, L), vm(2, 2, B, R, L), vm(nz, 2, R, L), vm(nd, 3, R, L),
                vm(X, R, L), vm(2, H, R, L), vm(R, L),
                vm(2, 3, R, L), vm(2, H, R, L), vm(nz, R, L), vm(nd, 2, R, L),
                pltpu.SemaphoreType.DMA((2,)),
                pltpu.SemaphoreType.DMA((messages,)),
                pltpu.SemaphoreType.DMA((messages,)),
            ],
            compiler_params=pltpu.CompilerParams(collective_id=0, has_side_effects=True),
        )(conserved, sigma_guess)

    specs = (P(None, "gx", "gy", "gz"), P("gx", "gy", "gz"))
    return jax.shard_map(on_device, mesh=mesh, in_specs=specs, out_specs=specs, check_vma=False)
```
